128 devices in a mesh: row: 16 (over x_lo, z, core), col: 8 (over x_hi, y).
Axes of the slice: x: 4 (x_hi: 2, x_lo: 2; x = x_hi * 2 + x_lo), y: 4, z: 4, core: 2. Of those that a mesh axis runs over, the one named last changes fastest.
Arguments:
- psi: bfloat16 [4096, 4096], P(('row', 'col')), may hold values from -6 to 6
- hpsi: bfloat16 [4096, 4096], P(('row', 'col')), may hold values from -0.09375 to 0.09375
- eigvec: bfloat16 [2, 16, 128, 4, 8, 128], P(None, 'row', None, None, 'col'), may hold values from -0.09375 to 0.09375
Outputs:
- correlation_tiles: float32 [2, 16, 128, 4, 8, 128], P(None, 'row', None, None, 'col')
- updated_tiles: float32 [2, 16, 128, 4, 8, 128], P(None, 'row', None, None, 'col')
- diag_part: float32 [16], replicated
- offdiag_part: float32 [16], replicated
- rotated: bfloat16 [4096, 4, 8, 128], P('row', None, 'col')
The draws below stay inside these ranges and needn't reach their ends.
All inputs are finite; a program needn't handle non-finite values.
Results may differ from the reference program's by a relative error of at most 0.001.
Values may be sent and summed in bfloat16 or wider, within the bound.
A program may use at most 128 MiB of HBM per device.

```python
import jax
import jax.numpy as jnp
from jax import lax

NB = 4096
TB = 128
PB = 16
NG = 4096
KR = 2
KC = 4
N_ROW = 16
N_COL = 8


def block_levels(key, shape, pieces, least, largest):
    def one(position, shards_of):
        heights = jax.random.uniform(jax.random.fold_in(jax.random.fold_in(key, 6), position), (shards_of,), jnp.float32, least / len(pieces), largest / len(pieces))
        return jnp.repeat(jnp.exp(heights), shape[position] // shards_of).reshape((-1,) + (1,) * (len(shape) - position - 1))

    loudness = one(*pieces[0])
    for cut in pieces[1:]:
        loudness = loudness * one(*cut)
    return loudness


def centred(rng, dims, spread, most, pieces=(), held_as=jnp.bfloat16):
    array = jax.random.normal(rng, dims, jnp.float32) * spread
    if len(pieces) > 0:
        array = block_levels(rng, dims, pieces, -0.22, 0.18) * array
    return jnp.clip(array, min=-most, max=most).astype(held_as)


def setup_inputs(seed: int = 0) -> dict:
    splits = jax.random.split(jax.random.key(seed), 4)
    psi = centred(splits[0], (NG, NB), 1.0, 6.0, ((0, 128),))
    hpsi = centred(splits[1], (NG, NB), NG ** -0.5, 0.09375, ((0, 128),))
    eigvec = centred(splits[2], (KR, N_ROW, TB, KC, N_COL, TB), NB ** -0.5, 0.09375, ((1, 16), (4, 8)))
    return dict(psi=psi, hpsi=hpsi, eigvec=eigvec)


def reference(psi, hpsi, eigvec):
    highest = lax.Precision.HIGHEST
    mixed = jnp.dot(psi.T, hpsi, preferred_element_type=jnp.float32)
    reduced = 0.5 * (mixed + mixed.T)
    correlation = jnp.dot(psi.T, psi, preferred_element_type=jnp.float32) / float(NG)
    panel = reduced[:, :PB]
    positions = jnp.arange(NB)
    vecs = jnp.zeros((NB, PB), jnp.float32)
    images = jnp.zeros((NB, PB), jnp.float32)
    diag_list = []
    off_list = []
    for step in range(PB):
        column = panel[:, step] - jnp.dot(vecs, images[step], precision=highest) - jnp.dot(images, vecs[step], precision=highest)
        pivot = column[step + 1]
        below = positions > step + 1
        tail = jnp.sum(jnp.where(below, column * column, 0.0))
        length = jnp.sqrt(pivot * pivot + tail)
        beta = jnp.where(pivot >= 0.0, -length, length)
        tau = (beta - pivot) / beta
        vector = jnp.where(positions == step + 1, 1.0, jnp.where(below, column / (pivot - beta), 0.0))
        image = jnp.dot(reduced, vector, precision=highest)
        image = image - jnp.dot(vecs, jnp.dot(vector, images, precision=highest), precision=highest)
        image = image - jnp.dot(images, jnp.dot(vector, vecs, precision=highest), precision=highest)
        image = tau * image
        image = image - 0.5 * tau * jnp.dot(image, vector, precision=highest) * vector
        vecs = vecs.at[:, step].set(vector)
        images = images.at[:, step].set(image)
        diag_list.append(column[step])
        off_list.append(beta)
    updated = reduced - jnp.dot(vecs, images.T, precision=highest) - jnp.dot(images, vecs.T, precision=highest)
    rotation = eigvec.reshape(NB, NB)
    rotated = jnp.dot(psi, rotation, preferred_element_type=jnp.float32).astype(jnp.bfloat16)
    tile_shape = (KR, N_ROW, TB, KC, N_COL, TB)
    return (correlation.reshape(tile_shape), updated.reshape(tile_shape), jnp.stack(diag_list).astype(jnp.float32), jnp.stack(off_list).astype(jnp.float32), rotated.reshape(NG, KC, N_COL, TB))
```

```python
import jax
import jax.numpy as jnp
from jax import lax
from jax.experimental import pallas as pl
from jax.experimental.pallas import tpu as pltpu
from jax.sharding import PartitionSpec as P

PB = 16
MESH = pl.DeviceIdType.MESH


def in_one_piece(arrays, axis, split_dim, concat_dim, along):
    both = jnp.concatenate(arrays, axis=along)
    whole, at, gathered = (
        lax.all_to_all(both, axis, split_axis=split_dim, concat_axis=concat_dim, tiled=True),
        0,
        [],
    )
    for a in arrays:
        gathered.append(lax.slice_in_dim(whole, at, at + a.shape[along], axis=along))
        at += a.shape[along]
    return tuple(gathered)


def in_one_piece_2(arrays, axis, dim, along):
    both = jnp.concatenate(arrays, axis=along)
    whole, at, gathered = (lax.all_gather(both, axis, axis=dim, tiled=True), 0, [])
    for a in arrays:
        gathered.append(lax.slice_in_dim(whole, at, at + a.shape[along], axis=along))
        at += a.shape[along]
    return tuple(gathered)


def inner(left, right):
    return lax.dot_general(
        left, right, (((0,), (0,)), ((), ())), preferred_element_type=jnp.float32
    )


def split_three(x):
    high = x.astype(jnp.bfloat16)
    rest = x - high.astype(jnp.float32)
    mid = rest.astype(jnp.bfloat16)
    low = (rest - mid.astype(jnp.float32)).astype(jnp.bfloat16)
    return high, mid, low


def panel_kernel(
    a_ref,
    updated_ref,
    diag_ref,
    off_ref,
    panel_out,
    panel_in,
    panel,
    vecs,
    images,
    vec,
    lanes_sum,
    parts_out,
    parts_in,
    whole,
    send_sem,
    panel_sem,
    parts_sem,
):
    rows = lax.axis_size("row")
    cols = lax.axis_size("col")
    row = lax.axis_index("row")
    col = lax.axis_index("col")
    height = a_ref.shape[1]
    tile = 128
    blocks = a_ref.shape[2] // tile
    halves = height // tile
    tiles = rows * halves
    order = sorted(range(1, rows), key=lambda d: -min(d, rows - d))
    peers = [{"row": lax.rem(row + d, rows), "col": col} for d in order]
    barrier = pltpu.get_barrier_semaphore()
    for peer in peers:
        pl.semaphore_signal(barrier, inc=1, device_id=peer, device_id_type=MESH)
    pl.semaphore_wait(barrier, rows - 1)

    def to_peers(source, target, recv):
        for peer in peers:
            pltpu.make_async_remote_copy(
                src_ref=source,
                dst_ref=target,
                send_sem=send_sem,
                recv_sem=recv,
                device_id=peer,
                device_id_type=MESH,
            ).start()

    for half in range(halves):
        first = a_ref[0, half * tile : (half + 1) * tile, 0:tile]
        panel_out[:, half, :] = jnp.transpose(first)[0:PB, :]
    to_peers(panel_out, panel_in.at[row], panel_sem)
    panel_in[row] = panel_out[...]
    vecs[...] = jnp.zeros_like(vecs)
    images[...] = jnp.zeros_like(images)
    spot = lax.broadcasted_iota(jnp.int32, (tiles, tile), 0)
    lane = lax.broadcasted_iota(jnp.int32, (tiles, tile), 1)
    positions = ((spot % halves) * rows + spot // halves) * tile + lane
    slot = lax.broadcasted_iota(jnp.int32, (8, tile), 1)
    others = panel_in.at[pl.ds(0, rows - 1)]
    pltpu.make_async_copy(others, others, panel_sem).wait()
    for r in range(rows):
        panel[:, r * halves : (r + 1) * halves, :] = panel_in[r]

    def total(x):
        return jnp.sum(x, axis=(0, 1), keepdims=True)

    def totals(x):
        return jnp.sum(x, axis=(1, 2), keepdims=True)

    def reflector(column, step):
        at = total(jnp.where(positions == step, column, 0.0))
        pivot = total(jnp.where(positions == step + 1, column, 0.0))
        below = positions > step + 1
        tail = total(jnp.where(below, column * column, 0.0))
        length = jnp.sqrt(pivot * pivot + tail)
        beta = jnp.where(pivot >= 0.0, -length, length)
        tau = (beta - pivot) / beta
        vector = jnp.where(
            positions == step + 1, 1.0, jnp.where(below, column / (pivot - beta), 0.0)
        )
        return at, beta, tau, vector

    def advance(step, carry):
        column, diagonal, offdiag = carry
        at, beta, tau, vector = reflector(column, step)
        diagonal = jnp.where(slot == step, at, diagonal)
        offdiag = jnp.where(slot == step, beta, offdiag)
        vec[...] = vector
        spread = [jnp.broadcast_to(vec[e : e + 1, :], (8, tile)) for e in range(tiles)]

        def band(group, _):
            at_rows = pl.ds(pl.multiple_of(group * 8, 8), 8)
            sums = [jnp.zeros((8, tile), jnp.float32) for _ in range(4)]
            for e in range(tiles):
                t = (e % halves) * rows + e // halves
                b = t // cols
                block = a_ref[t % cols, at_rows, b * tile : (b + 1) * tile]
                sums[e % 4] = sums[e % 4] + block * spread[e]
            lanes_sum[at_rows, :] = (sums[0] + sums[1]) + (sums[2] + sums[3])
            return 0

        lax.fori_loop(0, height // 8, band, 0)
        ones = jnp.ones((16, tile), jnp.bfloat16)
        product = jnp.zeros((16, height), jnp.float32)
        for piece in split_three(lanes_sum[...]):
            product = product + lax.dot_general(
                ones, piece, (((1,), (1,)), ((), ())), preferred_element_type=jnp.float32
            )
        for half in range(halves):
            parts_out[step, half : half + 1, :] = product[0:1, half * tile : (half + 1) * tile]
        to_peers(parts_out.at[step], parts_in.at[step, row], parts_sem.at[step])
        parts_in[step, row] = parts_out[step]
        by_vecs = totals(vecs[...] * vector[None])
        by_images = totals(images[...] * vector[None])
        known = jnp.sum(vecs[...] * by_images + images[...] * by_vecs, axis=0)
        following = jnp.minimum(step + 1, PB - 1)
        here = positions == following
        head_v = totals(jnp.where(here[None], vecs[...], 0.0))
        head_w = totals(jnp.where(here[None], images[...], 0.0))
        ahead = panel[following] - jnp.sum(vecs[...] * head_w + images[...] * head_v, axis=0)
        vecs[step] = vector
        rest = parts_in.at[step, pl.ds(0, rows - 1)]
        pltpu.make_async_copy(rest, rest, parts_sem.at[step]).wait()
        for r in range(rows):
            whole[r * halves : (r + 1) * halves, :] = parts_in[step, r]
        image = tau * (whole[...] - known)
        image = image - 0.5 * tau * total(image * vector) * vector
        images[step] = image
        lead_v = total(jnp.where(here, vector, 0.0))
        lead_w = total(jnp.where(here, image, 0.0))
        column = ahead - vector * lead_w - image * lead_v
        return column, diagonal, offdiag

    nothing = jnp.zeros((8, tile), jnp.float32)
    _, diagonal, offdiag = lax.fori_loop(0, PB, advance, (panel[0], nothing, nothing))
    diag_ref[...] = diagonal
    off_ref[...] = offdiag
    left_v = [vecs[:, pl.ds(halves * row + h, 1), :].reshape(PB, tile) for h in range(halves)]
    left_w = [images[:, pl.ds(halves * row + h, 1), :].reshape(PB, tile) for h in range(halves)]
    for b in range(blocks):
        t = b * cols + col
        e = (t % rows) * halves + t // rows
        right_v = vecs[:, pl.ds(e, 1), :].reshape(PB, tile)
        right_w = images[:, pl.ds(e, 1), :].reshape(PB, tile)
        for h in range(halves):
            change = lax.dot_general(
                jnp.concatenate([left_v[h], left_w[h]], axis=0),
                jnp.concatenate([right_w, right_v], axis=0),
                (((0,), (0,)), ((), ())),
                precision=lax.Precision.HIGHEST,
                preferred_element_type=jnp.float32,
            )
            block = a_ref[col, h * tile : (h + 1) * tile, b * tile : (b + 1) * tile]
            updated_ref[pl.ds(h * tile * blocks + b, tile, stride=blocks), :] = block - change

    def drain(_, carry):
        pltpu.make_async_copy(parts_out.at[0], parts_out.at[0], send_sem).wait()
        return carry

    for _ in peers:
        pltpu.make_async_copy(panel_out, panel_out, send_sem).wait()
    lax.fori_loop(0, PB * (rows - 1), drain, 0)


def reduce_panel(a_rows, rows):
    cols, height, width = a_rows.shape
    tile = 128
    halves = height // tile
    tiles = rows * halves
    vmem = pl.BlockSpec(memory_space=pltpu.VMEM)
    return pl.pallas_call(
        panel_kernel,
        out_shape=(
            jax.ShapeDtypeStruct((height * width // tile, tile), jnp.float32),
            jax.ShapeDtypeStruct((8, tile), jnp.float32),
            jax.ShapeDtypeStruct((8, tile), jnp.float32),
        ),
        in_specs=[vmem],
        out_specs=(vmem, vmem, vmem),
        scratch_shapes=[
            pltpu.VMEM((PB, halves, tile), jnp.float32),
            pltpu.VMEM((rows, PB, halves, tile), jnp.float32),
            pltpu.VMEM((PB, tiles, tile), jnp.float32),
            pltpu.VMEM((PB, tiles, tile), jnp.float32),
            pltpu.VMEM((PB, tiles, tile), jnp.float32),
            pltpu.VMEM((tiles, tile), jnp.float32),
            pltpu.VMEM((height, tile), jnp.float32),
            pltpu.VMEM((PB, halves, tile), jnp.float32),
            pltpu.VMEM((PB, rows, halves, tile), jnp.float32),
            pltpu.VMEM((tiles, tile), jnp.float32),
            pltpu.SemaphoreType.DMA,
            pltpu.SemaphoreType.DMA,
            pltpu.SemaphoreType.DMA((PB,)),
        ],
        compiler_params=pltpu.CompilerParams(
            collective_id=0, has_side_effects=True, vmem_limit_bytes=48 * 1024 * 1024
        ),
        name="panel",
    )(a_rows)


def on_device(psi, hpsi, eigvec):
    g_rows = psi.shape[0]
    row_tiles = eigvec.shape[0]
    tile_size = eigvec.shape[2]
    col_tiles = eigvec.shape[3]
    row_count = lax.axis_size("row")
    col_count = lax.axis_size("col")
    gvecs = g_rows * row_count * col_count
    row_width = row_tiles * tile_size
    col_width = col_tiles * tile_size
    lifted = (
        psi.reshape(1, g_rows, row_tiles, row_count, tile_size),
        hpsi.reshape(1, g_rows, row_tiles, row_count, tile_size),
    )
    swapped = in_one_piece((lifted[0], lifted[1]), "row", 3, 0, 1)
    joined = in_one_piece_2((swapped[0], swapped[1]), "col", 1, 0)
    psi_rows = joined[0].reshape(gvecs, row_width)
    hpsi_rows = joined[1].reshape(gvecs, row_width)
    lowered = (
        psi.reshape(g_rows, col_tiles, col_count, tile_size),
        hpsi.reshape(g_rows, col_tiles, col_count, tile_size),
    )
    moved = in_one_piece((lowered[0], lowered[1]), "col", 2, 0, 1)
    stacked = in_one_piece_2((moved[0], moved[1]), "row", 0, 1)
    psi_cols = stacked[0].reshape(gvecs, col_width)
    hpsi_cols = stacked[1].reshape(gvecs, col_width)
    reduced = 0.5 * (inner(psi_rows, hpsi_cols) + inner(hpsi_rows, psi_cols))
    correlation = inner(psi_rows, psi_cols) / float(gvecs)
    a_rows = lax.all_gather(reduced, "col")
    updated, diagonal, offdiag = reduce_panel(a_rows, row_count)
    flat = eigvec.reshape(row_width, col_width)
    rotated = lax.psum_scatter(
        jnp.dot(psi_rows, flat, preferred_element_type=jnp.float32),
        "row",
        scatter_dimension=0,
        tiled=True,
    )
    tile_shape = (row_tiles, 1, tile_size, col_tiles, 1, tile_size)
    return (
        correlation.reshape(tile_shape),
        updated.reshape(tile_shape),
        diagonal[0, :PB],
        offdiag[0, :PB],
        rotated.astype(jnp.bfloat16).reshape(rotated.shape[0], col_tiles, 1, tile_size),
    )


def solution(mesh):
    return jax.shard_map(
        on_device,
        mesh=mesh,
        in_specs=(
            P(("row", "col"), None),
            P(("row", "col"), None),
            P(None, "row", None, None, "col", None),
        ),
        out_specs=(
            P(None, "row", None, None, "col", None),
            P(None, "row", None, None, "col", None),
            P(),
            P(),
            P("row", None, "col", None),
        ),
        check_vma=False,
    )
```

```python
import jax
import jax.numpy as jnp
from jax import lax
from jax.experimental import pallas as pl
from jax.experimental.pallas import tpu as pltpu
from jax.sharding import PartitionSpec as P

PB = 16
MESH = pl.DeviceIdType.MESH


def split_three(x):
    high = x.astype(jnp.bfloat16)
    rest = x - high.astype(jnp.float32)
    mid = rest.astype(jnp.bfloat16)
    low = (rest - mid.astype(jnp.float32)).astype(jnp.bfloat16)
    return high, mid, low


def panel_kernel(
    a_ref,
    updated_ref,
    diag_ref,
    off_ref,
    panel_out,
    panel_in,
    panel,
    vecs,
    images,
    vec,
    lanes_sum,
    parts_out,
    parts_in,
    whole,
    send_sem,
    panel_sem,
    parts_sem,
):
    rows = lax.axis_size("row")
    cols = lax.axis_size("col")
    row = lax.axis_index("row")
    col = lax.axis_index("col")
    height = a_ref.shape[1]
    tile = 128
    blocks = a_ref.shape[2] // tile
    halves = height // tile
    tiles = rows * halves
    order = sorted(range(1, rows), key=lambda d: -min(d, rows - d))
    peers = [{"row": lax.rem(row + d, rows), "col": col} for d in order]
    barrier = pltpu.get_barrier_semaphore()
    for peer in peers:
        pl.semaphore_signal(barrier, inc=1, device_id=peer, device_id_type=MESH)
    pl.semaphore_wait(barrier, rows - 1)

    def to_peers(source, target, recv):
        for peer in peers:
            pltpu.make_async_remote_copy(
                src_ref=source,
                dst_ref=target,
                send_sem=send_sem,
                recv_sem=recv,
                device_id=peer,
                device_id_type=MESH,
            ).start()

    for half in range(halves):
        first = a_ref[0, half * tile : (half + 1) * tile, 0:tile]
        panel_out[:, half, :] = jnp.transpose(first)[0:PB, :]
    to_peers(panel_out, panel_in.at[row], panel_sem)
    panel_in[row] = panel_out[...]
    vecs[...] = jnp.zeros_like(vecs)
    images[...] = jnp.zeros_like(images)
    spot = lax.broadcasted_iota(jnp.int32, (tiles, tile), 0)
    lane = lax.broadcasted_iota(jnp.int32, (tiles, tile), 1)
    positions = ((spot % halves) * rows + spot // halves) * tile + lane
    slot = lax.broadcasted_iota(jnp.int32, (8, tile), 1)
    others = panel_in.at[pl.ds(0, rows - 1)]
    pltpu.make_async_copy(others, others, panel_sem).wait()
    for r in range(rows):
        panel[:, r * halves : (r + 1) * halves, :] = panel_in[r]

    def total(x):
        return jnp.sum(x, axis=(0, 1), keepdims=True)

    def totals(x):
        return jnp.sum(x, axis=(1, 2), keepdims=True)

    def reflector(column, step):
        at = total(jnp.where(positions == step, column, 0.0))
        pivot = total(jnp.where(positions == step + 1, column, 0.0))
        below = positions > step + 1
        tail = total(jnp.where(below, column * column, 0.0))
        length = jnp.sqrt(pivot * pivot + tail)
        beta = jnp.where(pivot >= 0.0, -length, length)
        tau = (beta - pivot) / beta
        vector = jnp.where(
            positions == step + 1, 1.0, jnp.where(below, column / (pivot - beta), 0.0)
        )
        return at, beta, tau, vector

    def advance(step, carry):
        column, diagonal, offdiag = carry
        at, beta, tau, vector = reflector(column, step)
        diagonal = jnp.where(slot == step, at, diagonal)
        offdiag = jnp.where(slot == step, beta, offdiag)
        vec[...] = vector
        spread = [jnp.broadcast_to(vec[e : e + 1, :], (8, tile)) for e in range(tiles)]

        def band(group, _):
            at_rows = pl.ds(pl.multiple_of(group * 8, 8), 8)
            sums = [jnp.zeros((8, tile), jnp.float32) for _ in range(4)]
            for e in range(tiles):
                t = (e % halves) * rows + e // halves
                b = t // cols
                block = a_ref[t % cols, at_rows, b * tile : (b + 1) * tile]
                sums[e % 4] = sums[e % 4] + block * spread[e]
            lanes_sum[at_rows, :] = (sums[0] + sums[1]) + (sums[2] + sums[3])
            return 0

        lax.fori_loop(0, height // 8, band, 0)
        ones = jnp.ones((16, tile), jnp.bfloat16)
        product = jnp.zeros((16, height), jnp.float32)
        for piece in split_three(lanes_sum[...]):
            product = product + lax.dot_general(
                ones, piece, (((1,), (1,)), ((), ())), preferred_element_type=jnp.float32
            )
        for half in range(halves):
            parts_out[step, half : half + 1, :] = product[0:1, half * tile : (half + 1) * tile]
        to_peers(parts_out.at[step], parts_in.at[step, row], parts_sem.at[step])
        parts_in[step, row] = parts_out[step]
        by_vecs = totals(vecs[...] * vector[None])
        by_images = totals(images[...] * vector[None])
        known = jnp.sum(vecs[...] * by_images + images[...] * by_vecs, axis=0)
        following = jnp.minimum(step + 1, PB - 1)
        here = positions == following
        head_v = totals(jnp.where(here[None], vecs[...], 0.0))
        head_w = totals(jnp.where(here[None], images[...], 0.0))
        ahead = panel[following] - jnp.sum(vecs[...] * head_w + images[...] * head_v, axis=0)
        vecs[step] = vector
        rest = parts_in.at[step, pl.ds(0, rows - 1)]
        pltpu.make_async_copy(rest, rest, parts_sem.at[step]).wait()
        for r in range(rows):
            whole[r * halves : (r + 1) * halves, :] = parts_in[step, r]
        image = tau * (whole[...] - known)
        image = image - 0.5 * tau * total(image * vector) * vector
        images[step] = image
        lead_v = total(jnp.where(here, vector, 0.0))
        lead_w = total(jnp.where(here, image, 0.0))
        column = ahead - vector * lead_w - image * lead_v
        return column, diagonal, offdiag

    nothing = jnp.zeros((8, tile), jnp.float32)
    _, diagonal, offdiag = lax.fori_loop(0, PB, advance, (panel[0], nothing, nothing))
    diag_ref[...] = diagonal
    off_ref[...] = offdiag
    left_v = [vecs[:, pl.ds(halves * row + h, 1), :].reshape(PB, tile) for h in range(halves)]
    left_w = [images[:, pl.ds(halves * row + h, 1), :].reshape(PB, tile) for h in range(halves)]
    for b in range(blocks):
        t = b * cols + col
        e = (t % rows) * halves + t // rows
        right_v = vecs[:, pl.ds(e, 1), :].reshape(PB, tile)
        right_w = images[:, pl.ds(e, 1), :].reshape(PB, tile)
        for h in range(halves):
            change = lax.dot_general(
                jnp.concatenate([left_v[h], left_w[h]], axis=0),
                jnp.concatenate([right_w, right_v], axis=0),
                (((0,), (0,)), ((), ())),
                precision=lax.Precision.HIGHEST,
                preferred_element_type=jnp.float32,
            )
            block = a_ref[col, h * tile : (h + 1) * tile, b * tile : (b + 1) * tile]
            updated_ref[pl.ds(h * tile * blocks + b, tile, stride=blocks), :] = block - change

    def drain(_, carry):
        pltpu.make_async_copy(parts_out.at[0], parts_out.at[0], send_sem).wait()
        return carry

    for _ in peers:
        pltpu.make_async_copy(panel_out, panel_out, send_sem).wait()
    lax.fori_loop(0, PB * (rows - 1), drain, 0)


def reduce_panel(a_rows, rows):
    cols, height, width = a_rows.shape
    tile = 128
    halves = height // tile
    tiles = rows * halves
    vmem = pl.BlockSpec(memory_space=pltpu.VMEM)
    return pl.pallas_call(
        panel_kernel,
        out_shape=(
            jax.ShapeDtypeStruct((height * width // tile, tile), jnp.float32),
            jax.ShapeDtypeStruct((8, tile), jnp.float32),
            jax.ShapeDtypeStruct((8, tile), jnp.float32),
        ),
        in_specs=[vmem],
        out_specs=(vmem, vmem, vmem),
        scratch_shapes=[
            pltpu.VMEM((PB, halves, tile), jnp.float32),
            pltpu.VMEM((rows, PB, halves, tile), jnp.float32),
            pltpu.VMEM((PB, tiles, tile), jnp.float32),
            pltpu.VMEM((PB, tiles, tile), jnp.float32),
            pltpu.VMEM((PB, tiles, tile), jnp.float32),
            pltpu.VMEM((tiles, tile), jnp.float32),
            pltpu.VMEM((height, tile), jnp.float32),
            pltpu.VMEM((PB, halves, tile), jnp.float32),
            pltpu.VMEM((PB, rows, halves, tile), jnp.float32),
            pltpu.VMEM((tiles, tile), jnp.float32),
            pltpu.SemaphoreType.DMA,
            pltpu.SemaphoreType.DMA,
            pltpu.SemaphoreType.DMA((PB,)),
        ],
        compiler_params=pltpu.CompilerParams(
            collective_id=0, has_side_effects=True, vmem_limit_bytes=48 * 1024 * 1024
        ),
        name="panel",
    )(a_rows)


def lattice(row, col):
    pair = {"row": lax.div(row, 8), "col": lax.div(col, 4)}
    ring = {"row": lax.rem(lax.div(row, 2), 4), "col": lax.rem(col, 4)}
    return pair, ring


def front_kernel(
    psi_ref,
    hpsi_ref,
    a_ref,
    corr_ref,
    by_row,
    by_col,
    total_a,
    total_s,
    send_sem,
    swap_sem,
    ring_sem,
    core_sem,
):
    rows = lax.axis_size("row")
    cols = lax.axis_size("col")
    row = lax.axis_index("row")
    col = lax.axis_index("col")
    tile = 128
    halves = by_row.shape[4] // tile
    blocks = by_col.shape[4] // tile
    pair, ring = lattice(row, col)
    core = lax.rem(row, 2)
    inputs = (psi_ref, hpsi_ref)

    def place(axis, across, along):
        p = lax.rem(pair[axis] + across, 2)
        q = lax.rem(ring[axis] + along + 4, 4)
        return p * 8 + q * 2 + core if axis == "row" else p * 4 + q

    row_order = sorted(range(1, rows), key=lambda d: -min(d, rows - d))
    row_peers = [lax.rem(row + d, rows) for d in row_order]
    col_peers = [lax.rem(col + d, cols) for d in range(1, cols)]
    barrier = pltpu.get_barrier_semaphore()
    for r in row_peers:
        pl.semaphore_signal(
            barrier, inc=1, device_id={"row": r, "col": col}, device_id_type=MESH
        )
    for c in col_peers:
        pl.semaphore_signal(
            barrier, inc=1, device_id={"row": row, "col": c}, device_id_type=MESH
        )
    pl.semaphore_wait(barrier, rows + cols - 2)

    def send(source, target, sem, where):
        pltpu.make_async_remote_copy(
            src_ref=source,
            dst_ref=target,
            send_sem=send_sem,
            recv_sem=sem,
            device_id={"row": row, "col": col, **where},
            device_id_type=MESH,
        ).start()

    def lanes(tile_index):
        return pl.ds(pl.multiple_of(tile_index * tile, tile), tile)

    for n, source in enumerate(inputs):
        for r in row_peers:
            for h in range(halves):
                send(
                    source.at[:, lanes(h * rows + r)],
                    by_row.at[n, col, row, :, h * tile : (h + 1) * tile],
                    swap_sem.at[n, 0],
                    {"row": r},
                )
        for c in col_peers:
            for b in range(blocks):
                send(
                    source.at[:, lanes(b * cols + c)],
                    by_col.at[n, row, col, :, b * tile : (b + 1) * tile],
                    swap_sem.at[n, 1],
                    {"col": c},
                )
    for n, source in enumerate(inputs):
        for h in range(halves):
            by_row[n, col, row, :, h * tile : (h + 1) * tile] = source[:, lanes(h * rows + row)]
        for b in range(blocks):
            by_col[n, row, col, :, b * tile : (b + 1) * tile] = source[:, lanes(b * cols + col)]

    def arrived(ref, sem):
        pltpu.make_async_copy(ref, ref, sem).wait()

    kinds = [(n, part) for n in range(2) for part in range(2)]
    axes = ("col", "row")
    held = (by_row, by_col)

    def piece(n, part, across, along, half=None):
        whole = held[part].at[n, place(axes[part], across, along)]
        if half is None:
            return whole
        size = whole.shape[0] // 2
        return whole.at[pl.ds(half * size, size)]

    def along_ring(n, part, across, along, way, half, sem):
        what = piece(n, part, across, along, half)
        where = {axes[part]: place(axes[part], 0, way)}
        send(what, what, ring_sem.at[n, part, sem], where)

    def to_core(n, part, across, along, half=None):
        if part == 1:
            what = piece(n, part, across, along, half)
            send(what, what, core_sem.at[n], {"row": row + 1 - 2 * core})

    def wait_ring(n, part, across, along, half, sem):
        arrived(piece(n, part, across, along, half), ring_sem.at[n, part, sem])

    for n, part in kinds:
        count = (rows if part == 0 else cols) - 1
        mine = (col if part == 0 else row,)
        arrived(held[part].at[n, mine[0], pl.ds(0, count)], swap_sem.at[n, part])
        along_ring(n, part, 0, 0, 1, None, 0)
        along_ring(n, part, 0, 0, -1, None, 1)
        what = piece(n, part, 0, 0)
        send(what, what, ring_sem.at[n, part, 2], {axes[part]: place(axes[part], 1, 0)})
        to_core(n, part, 0, 0)
    for n, part in kinds:
        wait_ring(n, part, 0, -1, None, 0)
        along_ring(n, part, 0, -1, 1, 0, 3)
        to_core(n, part, 0, -1)
        wait_ring(n, part, 0, 1, None, 1)
        along_ring(n, part, 0, 1, -1, 1, 4)
        to_core(n, part, 0, 1)
        wait_ring(n, part, 1, 0, None, 2)
        along_ring(n, part, 1, 0, 1, None, 5)
        along_ring(n, part, 1, 0, -1, None, 6)
        to_core(n, part, 1, 0)
    for n, part in kinds:
        wait_ring(n, part, 0, 2, 0, 3)
        to_core(n, part, 0, 2, 0)
        wait_ring(n, part, 0, 2, 1, 4)
        to_core(n, part, 0, 2, 1)
        wait_ring(n, part, 1, -1, None, 5)
        along_ring(n, part, 1, -1, 1, 0, 7)
        to_core(n, part, 1, -1)
        wait_ring(n, part, 1, 1, None, 6)
        along_ring(n, part, 1, 1, -1, 1, 8)
        to_core(n, part, 1, 1)
    for n, part in kinds:
        wait_ring(n, part, 1, 2, 0, 7)
        to_core(n, part, 1, 2, 0)
        wait_ring(n, part, 1, 2, 1, 8)
        to_core(n, part, 1, 2, 1)
    for n in range(2):
        arrived(by_col.at[n, pl.ds(0, rows // 2)], core_sem.at[n])

    total_a[...] = jnp.zeros_like(total_a)
    total_s[...] = jnp.zeros_like(total_s)

    def product(left, right):
        return lax.dot_general(
            left, right, (((0,), (0,)), ((), ())), preferred_element_type=jnp.float32
        )

    def add(c, carry):
        depth = rows * by_row.shape[3]
        psi_r = by_row[0, c].reshape(depth, halves * tile)
        hpsi_r = by_row[1, c].reshape(depth, halves * tile)
        psi_c = by_col[0, :, c].reshape(depth, blocks * tile)
        hpsi_c = by_col[1, :, c].reshape(depth, blocks * tile)
        total_a[...] += product(psi_r, hpsi_c) + product(hpsi_r, psi_c)
        total_s[...] += product(psi_r, psi_c)
        return carry

    lax.fori_loop(0, cols, add, 0)
    gvecs = rows * cols * by_row.shape[3]
    a_ref[...] = 0.5 * total_a[...]
    for b in range(blocks):
        corr_ref[pl.ds(b, halves * tile, stride=blocks), :] = total_s[
            :, b * tile : (b + 1) * tile
        ] * (1.0 / gvecs)

    def sent(ref):
        pltpu.make_async_copy(ref, ref, send_sem).wait()

    for n in range(2):
        sent(by_row.at[n, 0, pl.ds(0, rows - 1)])
        sent(by_col.at[n, 0, pl.ds(0, cols - 1)])
        for part in range(2):
            for _ in range(5):
                sent(held[part].at[n, 0])
            for _ in range(2):
                sent(held[part].at[n, 0])
        sent(by_col.at[n, pl.ds(0, rows // 2)])


def reduce_front(psi, hpsi, rows, cols, halves, blocks):
    tile = 128
    vmem = pl.BlockSpec(memory_space=pltpu.VMEM)
    height, width = halves * tile, blocks * tile
    return pl.pallas_call(
        front_kernel,
        out_shape=(
            jax.ShapeDtypeStruct((height, width), jnp.float32),
            jax.ShapeDtypeStruct((height * blocks, tile), jnp.float32),
        ),
        in_specs=[vmem, vmem],
        out_specs=(vmem, vmem),
        scratch_shapes=[
            pltpu.VMEM((2, cols, rows, psi.shape[0], height), psi.dtype),
            pltpu.VMEM((2, rows, cols, psi.shape[0], width), psi.dtype),
            pltpu.VMEM((height, width), jnp.float32),
            pltpu.VMEM((height, width), jnp.float32),
            pltpu.SemaphoreType.DMA,
            pltpu.SemaphoreType.DMA((2, 2)),
            pltpu.SemaphoreType.DMA((2, 2, 9)),
            pltpu.SemaphoreType.DMA((2,)),
        ],
        compiler_params=pltpu.CompilerParams(
            collective_id=1, has_side_effects=True, vmem_limit_bytes=48 * 1024 * 1024
        ),
        name="front",
    )(psi, hpsi)


def on_device(psi, hpsi, eigvec):
    row_tiles, _, tile_size, col_tiles = eigvec.shape[:4]
    row_count = lax.axis_size("row")
    col_count = lax.axis_size("col")
    reduced, correlation = reduce_front(psi, hpsi, row_count, col_count, row_tiles, col_tiles)
    reduced, psi, eigvec = lax.optimization_barrier((reduced, psi, eigvec))
    a_rows = lax.all_gather(reduced, "col")
    psi_rows = lax.all_gather(psi, "col", axis=0, tiled=True)
    rotation = lax.all_gather(eigvec, "row", axis=1, tiled=True)
    updated, diagonal, offdiag = reduce_panel(a_rows, row_count)
    rotated = jnp.dot(
        psi_rows,
        rotation.reshape(psi.shape[1], col_tiles * tile_size),
        preferred_element_type=jnp.float32,
    )
    tile_shape = (row_tiles, 1, tile_size, col_tiles, 1, tile_size)
    return (
        correlation.reshape(tile_shape),
        updated.reshape(tile_shape),
        diagonal[0, :PB],
        offdiag[0, :PB],
        rotated.astype(jnp.bfloat16).reshape(rotated.shape[0], col_tiles, 1, tile_size),
    )


def solution(mesh):
    return jax.shard_map(
        on_device,
        mesh=mesh,
        in_specs=(
            P(("row", "col"), None),
            P(("row", "col"), None),
            P(None, "row", None, None, "col", None),
        ),
        out_specs=(
            P(None, "row", None, None, "col", None),
            P(None, "row", None, None, "col", None),
            P(),
            P(),
            P("row", None, "col", None),
        ),
        check_vma=False,
    )
```

```python
import jax
import jax.numpy as jnp
from jax import lax
from jax.experimental import pallas as pl
from jax.experimental.pallas import tpu as pltpu
from jax.sharding import PartitionSpec as P

PB = 16
MESH = pl.DeviceIdType.MESH


def split_three(x):
    high = x.astype(jnp.bfloat16)
    rest = x - high.astype(jnp.float32)
    mid = rest.astype(jnp.bfloat16)
    low = (rest - mid.astype(jnp.float32)).astype(jnp.bfloat16)
    return high, mid, low


def panel_kernel(
    a_ref,
    psi_ref,
    eig_ref,
    updated_ref,
    diag_ref,
    off_ref,
    rotated_ref,
    psi_rows,
    eig_cols,
    rotated,
    rotated_tiles,
    a_plane,
    panel_in,
    panel,
    vecs,
    images,
    vec,
    lanes_sum,
    parts_out,
    parts_in,
    whole,
    send_sem,
    ring_sem,
    panel_sem,
    parts_sem,
    eig_sem,
    core_sem,
    psi_sem,
):
    rows = lax.axis_size("row")
    cols = lax.axis_size("col")
    row = lax.axis_index("row")
    col = lax.axis_index("col")
    height = a_ref.shape[0]
    tile = 128
    blocks = a_ref.shape[1] // tile
    halves = height // tile
    tiles = rows * halves
    turns = cols // 2
    pair = lax.div(col, turns)
    ring = lax.rem(col, turns)
    order = sorted(
        ((d, e) for d in range(rows) for e in range(2) if d + e > 0),
        key=lambda de: -min(de[0], rows - de[0]) - 4 * de[1],
    )
    peers = [
        {"row": lax.rem(row + d, rows), "col": lax.rem(pair + e, 2) * turns + ring}
        for d, e in order
    ]
    around = [{"row": row, "col": pair * turns + lax.rem(ring + d, turns)} for d in (1, 3, 2)]
    barrier = pltpu.get_barrier_semaphore()
    for peer in peers + around:
        pl.semaphore_signal(barrier, inc=1, device_id=peer, device_id_type=MESH)
    pl.semaphore_wait(barrier, len(peers) + len(around))

    def send(source, target, recv, peer):
        pltpu.make_async_remote_copy(
            src_ref=source,
            dst_ref=target,
            send_sem=send_sem,
            recv_sem=recv,
            device_id=peer,
            device_id_type=MESH,
        ).start()

    def to_peers(source, target, recv):
        for peer in peers:
            send(source, target, recv, peer)

    def arrived(ref, sem):
        pltpu.make_async_copy(ref, ref, sem).wait()

    @pl.when(col == 0)
    def _():
        for half in range(halves):
            first = a_ref[half * tile : (half + 1) * tile, 0:tile]
            panel_in[row, :, half, :] = jnp.transpose(first)[0:PB, :]
        for peer in around:
            send(panel_in.at[row], panel_in.at[row], panel_sem.at[0], peer)

    above, below = lax.rem(ring + 1, turns), lax.rem(ring + turns - 1, turns)
    send(a_ref, a_plane.at[ring], ring_sem.at[0], around[0])
    send(a_ref, a_plane.at[ring], ring_sem.at[1], around[1])

    row_pair, row_ring, core = lax.div(row, 8), lax.rem(lax.div(row, 2), 4), lax.rem(row, 2)

    def eig_place(across, along):
        p = lax.rem(row_pair + across, 2)
        return p * 8 + lax.rem(row_ring + along + 4, 4) * 2 + core

    def psi_place(across, along):
        return lax.rem(pair + across, 2) * turns + lax.rem(ring + along + turns, turns)

    def piece(held, index, half):
        whole = held.at[index]
        if half is None:
            return whole
        size = whole.shape[0] // 2
        return whole.at[pl.ds(half * size, size)]

    def eig_send(across, along, way, half, sem):
        what = piece(eig_cols, eig_place(across, along), half)
        to = eig_place(1, 0) if way is None else eig_place(0, way)
        send(what, what, eig_sem.at[sem], {"row": to, "col": col})

    def eig_core(across, along, half):
        what = piece(eig_cols, eig_place(across, along), half)
        send(what, what, core_sem, {"row": row + 1 - 2 * core, "col": col})

    def eig_wait(across, along, half, sem):
        arrived(piece(eig_cols, eig_place(across, along), half), eig_sem.at[sem])

    def psi_send(across, along, way, half, sem):
        what = piece(psi_rows, psi_place(across, along), half)
        to = psi_place(1, 0) if way is None else psi_place(0, way)
        send(what, what, psi_sem.at[sem], {"row": row, "col": to})

    def psi_wait(across, along, half, sem):
        arrived(piece(psi_rows, psi_place(across, along), half), psi_sem.at[sem])

    eig_cols[row] = eig_ref[...]
    psi_rows[col] = psi_ref[...]
    eig_send(0, 0, 1, None, 0)
    eig_send(0, 0, -1, None, 1)
    eig_send(0, 0, None, None, 2)
    eig_core(0, 0, None)
    psi_send(0, 0, None, None, 2)

    @pl.when((pair == 0) & (ring > 0))
    def _():
        arrived(panel_in.at[row], panel_sem.at[0])

    @pl.when(pair == 0)
    def _():
        to_peers(panel_in.at[row], panel_in.at[row], panel_sem.at[1])

    a_plane[ring] = a_ref[...]
    vecs[...] = jnp.zeros_like(vecs)
    images[...] = jnp.zeros_like(images)
    spot = lax.broadcasted_iota(jnp.int32, (tiles, tile), 0)
    lane = lax.broadcasted_iota(jnp.int32, (tiles, tile), 1)
    positions = ((spot % halves) * rows + spot // halves) * tile + lane
    slot = lax.broadcasted_iota(jnp.int32, (8, tile), 1)

    @pl.when(pair == 0)
    def _():
        arrived(panel_in.at[pl.ds(0, rows - 1)], panel_sem.at[1])

    @pl.when(pair > 0)
    def _():
        arrived(panel_in, panel_sem.at[1])

    for r in range(rows):
        panel[:, r * halves : (r + 1) * halves, :] = panel_in[r]
    half_rows = height // 2
    arrived(a_plane.at[below], ring_sem.at[0])
    onward = a_plane.at[below, pl.ds(0, half_rows)]
    send(onward, onward, ring_sem.at[2], around[0])
    arrived(a_plane.at[above], ring_sem.at[1])
    back = a_plane.at[above, pl.ds(half_rows, half_rows)]
    send(back, back, ring_sem.at[3], around[1])
    eig_wait(0, -1, None, 0)
    eig_send(0, -1, 1, 0, 3)
    eig_core(0, -1, None)
    eig_wait(0, 1, None, 1)
    eig_send(0, 1, -1, 1, 4)
    eig_core(0, 1, None)
    eig_wait(1, 0, None, 2)
    eig_send(1, 0, 1, None, 5)
    eig_send(1, 0, -1, None, 6)
    eig_core(1, 0, None)
    psi_send(0, 0, 1, None, 0)
    psi_send(0, 0, -1, None, 1)
    psi_wait(1, 0, None, 2)
    psi_send(1, 0, 1, None, 5)
    psi_send(1, 0, -1, None, 6)
    across = lax.rem(ring + 2, turns)
    arrived(a_plane.at[across, pl.ds(0, half_rows)], ring_sem.at[2])
    arrived(a_plane.at[across, pl.ds(half_rows, half_rows)], ring_sem.at[3])

    def background(step):
        @pl.when(step == 0)
        def _():
            eig_wait(0, 2, 0, 3)
            eig_core(0, 2, 0)
            eig_wait(0, 2, 1, 4)
            eig_core(0, 2, 1)
            eig_wait(1, -1, None, 5)
            eig_send(1, -1, 1, 0, 7)
            eig_core(1, -1, None)
            eig_wait(1, 1, None, 6)
            eig_send(1, 1, -1, 1, 8)
            eig_core(1, 1, None)

        @pl.when(step == 2)
        def _():
            eig_wait(1, 2, 0, 7)
            eig_core(1, 2, 0)
            eig_wait(1, 2, 1, 8)
            eig_core(1, 2, 1)
            psi_wait(0, -1, None, 0)
            psi_send(0, -1, 1, 0, 3)
            psi_wait(0, 1, None, 1)
            psi_send(0, 1, -1, 1, 4)

        @pl.when(step == 4)
        def _():
            psi_wait(1, -1, None, 5)
            psi_send(1, -1, 1, 0, 7)
            psi_wait(1, 1, None, 6)
            psi_send(1, 1, -1, 1, 8)

        @pl.when(step == 7)
        def _():
            for half in range(2):
                psi_wait(0, 2, half, 3 + half)
                psi_wait(1, 2, half, 7 + half)
            arrived(eig_cols.at[pl.ds(0, rows // 2)], core_sem)
            rotated[...] = jnp.zeros_like(rotated)

        @pl.when(step >= PB // 2)
        def _():
            per = rows // (PB // 2)
            for k in range(per):
                r = (step - PB // 2) * per + k
                left = [
                    psi_rows[:, :, pl.ds(pl.multiple_of((h * rows + r) * tile, tile), tile)]
                    for h in range(halves)
                ]
                left = jnp.concatenate([x.reshape(-1, tile) for x in left], axis=1)
                rotated[...] += jnp.dot(
                    left, eig_cols[r], preferred_element_type=jnp.float32
                )

    def total(x):
        return jnp.sum(x, axis=(0, 1), keepdims=True)

    def totals(x):
        return jnp.sum(x, axis=(1, 2), keepdims=True)

    def reflector(column, step):
        at = total(jnp.where(positions == step, column, 0.0))
        pivot = total(jnp.where(positions == step + 1, column, 0.0))
        under = positions > step + 1
        tail = total(jnp.where(under, column * column, 0.0))
        length = jnp.sqrt(pivot * pivot + tail)
        beta = jnp.where(pivot >= 0.0, -length, length)
        tau = (beta - pivot) / beta
        vector = jnp.where(
            positions == step + 1, 1.0, jnp.where(under, column / (pivot - beta), 0.0)
        )
        return at, beta, tau, vector

    def advance(step, carry):
        column, diagonal, offdiag = carry
        at, beta, tau, vector = reflector(column, step)
        diagonal = jnp.where(slot == step, at, diagonal)
        offdiag = jnp.where(slot == step, beta, offdiag)
        vec[...] = vector
        spread = []
        for y in range(turns):
            for b in range(blocks):
                t = b * cols + pair * turns + y
                e = lax.rem(t, rows) * halves + lax.div(t, rows)
                spread.append(jnp.broadcast_to(vec[pl.ds(e, 1), :], (8, tile)))

        def band(group, _):
            at_rows = pl.ds(pl.multiple_of(group * 8, 8), 8)
            sums = [jnp.zeros((8, tile), jnp.float32) for _ in range(4)]
            for y in range(turns):
                for b in range(blocks):
                    block = a_plane[y, at_rows, b * tile : (b + 1) * tile]
                    sums[b] = sums[b] + block * spread[y * blocks + b]
            lanes_sum[at_rows, :] = (sums[0] + sums[1]) + (sums[2] + sums[3])
            return 0

        lax.fori_loop(0, height // 8, band, 0)
        ones = jnp.ones((16, tile), jnp.bfloat16)
        product = jnp.zeros((16, height), jnp.float32)
        for piece in split_three(lanes_sum[...]):
            product = product + lax.dot_general(
                ones, piece, (((1,), (1,)), ((), ())), preferred_element_type=jnp.float32
            )
        for half in range(halves):
            parts_out[step, half : half + 1, :] = product[0:1, half * tile : (half + 1) * tile]
        to_peers(parts_out.at[step], parts_in.at[step, pair * rows + row], parts_sem.at[step])
        parts_in[step, pair * rows + row] = parts_out[step]
        background(step)
        by_vecs = totals(vecs[...] * vector[None])
        by_images = totals(images[...] * vector[None])
        known = jnp.sum(vecs[...] * by_images + images[...] * by_vecs, axis=0)
        following = jnp.minimum(step + 1, PB - 1)
        here = positions == following
        head_v = totals(jnp.where(here[None], vecs[...], 0.0))
        head_w = totals(jnp.where(here[None], images[...], 0.0))
        ahead = panel[following] - jnp.sum(vecs[...] * head_w + images[...] * head_v, axis=0)
        vecs[step] = vector
        arrived(parts_in.at[step, pl.ds(0, 2 * rows - 1)], parts_sem.at[step])
        for r in range(rows):
            whole[r * halves : (r + 1) * halves, :] = parts_in[step, r] + parts_in[step, rows + r]
        image = tau * (whole[...] - known)
        image = image - 0.5 * tau * total(image * vector) * vector
        images[step] = image
        lead_v = total(jnp.where(here, vector, 0.0))
        lead_w = total(jnp.where(here, image, 0.0))
        column = ahead - vector * lead_w - image * lead_v
        return column, diagonal, offdiag

    nothing = jnp.zeros((8, tile), jnp.float32)
    _, diagonal, offdiag = lax.fori_loop(0, PB, advance, (panel[0], nothing, nothing))
    diag_ref[...] = diagonal[0:1, 0:PB]
    off_ref[...] = offdiag[0:1, 0:PB]
    depth = rotated.shape[0]
    for b in range(blocks):
        rotated_tiles[pl.ds(b, depth, stride=blocks), :] = rotated[:, b * tile : (b + 1) * tile]
    rotated_ref[...] = rotated_tiles[...].astype(rotated_ref.dtype)
    left_v = [vecs[:, pl.ds(halves * row + h, 1), :].reshape(PB, tile) for h in range(halves)]
    left_w = [images[:, pl.ds(halves * row + h, 1), :].reshape(PB, tile) for h in range(halves)]
    for b in range(blocks):
        t = b * cols + col
        e = (t % rows) * halves + t // rows
        right_v = vecs[:, pl.ds(e, 1), :].reshape(PB, tile)
        right_w = images[:, pl.ds(e, 1), :].reshape(PB, tile)
        for h in range(halves):
            change = lax.dot_general(
                jnp.concatenate([left_v[h], left_w[h]], axis=0),
                jnp.concatenate([right_w, right_v], axis=0),
                (((0,), (0,)), ((), ())),
                precision=lax.Precision.HIGHEST,
                preferred_element_type=jnp.float32,
            )
            block = a_ref[h * tile : (h + 1) * tile, b * tile : (b + 1) * tile]
            updated_ref[pl.ds(h * tile * blocks + b, tile, stride=blocks), :] = block - change


    def sent(ref):
        pltpu.make_async_copy(ref, ref, send_sem).wait()

    @pl.when(col == 0)
    def _():
        sent(panel_in.at[pl.ds(0, len(around))])

    @pl.when(pair == 0)
    def _():
        sent(panel_in.at[pl.ds(0, rows)])
        sent(panel_in.at[pl.ds(0, rows - 1)])

    for _ in range(3):
        sent(a_ref)
    sent(eig_cols.at[pl.ds(0, 7)])
    sent(eig_cols.at[pl.ds(0, rows // 2)])
    sent(psi_rows.at[pl.ds(0, 7)])

    def drain(step, carry):
        sent(parts_in.at[step, pl.ds(0, 2 * rows - 1)])
        return carry

    lax.fori_loop(0, PB, drain, 0)


def reduce_panel(block, psi, eigvec, rows, cols):
    height, width = block.shape
    tile = 128
    halves = height // tile
    tiles = rows * halves
    depth = cols * psi.shape[0]
    vmem = pl.BlockSpec(memory_space=pltpu.VMEM)
    return pl.pallas_call(
        panel_kernel,
        out_shape=(
            jax.ShapeDtypeStruct((height * width // tile, tile), jnp.float32),
            jax.ShapeDtypeStruct((1, PB), jnp.float32),
            jax.ShapeDtypeStruct((1, PB), jnp.float32),
            jax.ShapeDtypeStruct((depth * width // tile, tile), psi.dtype),
        ),
        in_specs=[vmem, vmem, vmem],
        out_specs=(vmem, vmem, vmem, vmem),
        scratch_shapes=[
            pltpu.VMEM((cols, *psi.shape), psi.dtype),
            pltpu.VMEM((rows, *eigvec.shape), eigvec.dtype),
            pltpu.VMEM((depth, width), jnp.float32),
            pltpu.VMEM((depth * width // tile, tile), jnp.float32),
            pltpu.VMEM((cols // 2, height, width), jnp.float32),
            pltpu.VMEM((rows, PB, halves, tile), jnp.float32),
            pltpu.VMEM((PB, tiles, tile), jnp.float32),
            pltpu.VMEM((PB, tiles, tile), jnp.float32),
            pltpu.VMEM((PB, tiles, tile), jnp.float32),
            pltpu.VMEM((tiles, tile), jnp.float32),
            pltpu.VMEM((height, tile), jnp.float32),
            pltpu.VMEM((PB, halves, tile), jnp.float32),
            pltpu.VMEM((PB, 2 * rows, halves, tile), jnp.float32),
            pltpu.VMEM((tiles, tile), jnp.float32),
            pltpu.SemaphoreType.DMA,
            pltpu.SemaphoreType.DMA((4,)),
            pltpu.SemaphoreType.DMA((2,)),
            pltpu.SemaphoreType.DMA((PB,)),
            pltpu.SemaphoreType.DMA((9,)),
            pltpu.SemaphoreType.DMA,
            pltpu.SemaphoreType.DMA((9,)),
        ],
        compiler_params=pltpu.CompilerParams(
            collective_id=0, has_side_effects=True, vmem_limit_bytes=48 * 1024 * 1024
        ),
        name="panel",
    )(block, psi, eigvec)


def lattice(row, col):
    pair = {"row": lax.div(row, 8), "col": lax.div(col, 4)}
    ring = {"row": lax.rem(lax.div(row, 2), 4), "col": lax.rem(col, 4)}
    return pair, ring


def front_kernel(
    psi_ref,
    hpsi_ref,
    a_ref,
    corr_ref,
    by_row,
    by_col,
    total_a,
    total_s,
    send_sem,
    swap_sem,
    ring_sem,
    core_sem,
):
    rows = lax.axis_size("row")
    cols = lax.axis_size("col")
    row = lax.axis_index("row")
    col = lax.axis_index("col")
    tile = 128
    halves = by_row.shape[4] // tile
    blocks = by_col.shape[4] // tile
    pair, ring = lattice(row, col)
    core = lax.rem(row, 2)
    inputs = (psi_ref, hpsi_ref)

    def place(axis, across, along):
        p = lax.rem(pair[axis] + across, 2)
        q = lax.rem(ring[axis] + along + 4, 4)
        return p * 8 + q * 2 + core if axis == "row" else p * 4 + q

    row_order = sorted(range(1, rows), key=lambda d: -min(d, rows - d))
    row_peers = [lax.rem(row + d, rows) for d in row_order]
    col_peers = [lax.rem(col + d, cols) for d in range(1, cols)]
    barrier = pltpu.get_barrier_semaphore()
    for r in row_peers:
        pl.semaphore_signal(
            barrier, inc=1, device_id={"row": r, "col": col}, device_id_type=MESH
        )
    for c in col_peers:
        pl.semaphore_signal(
            barrier, inc=1, device_id={"row": row, "col": c}, device_id_type=MESH
        )
    pl.semaphore_wait(barrier, rows + cols - 2)

    def send(source, target, sem, where):
        pltpu.make_async_remote_copy(
            src_ref=source,
            dst_ref=target,
            send_sem=send_sem,
            recv_sem=sem,
            device_id={"row": row, "col": col, **where},
            device_id_type=MESH,
        ).start()

    def lanes(tile_index):
        return pl.ds(pl.multiple_of(tile_index * tile, tile), tile)

    for n, source in enumerate(inputs):
        for r in row_peers:
            for h in range(halves):
                send(
                    source.at[:, lanes(h * rows + r)],
                    by_row.at[n, col, row, :, h * tile : (h + 1) * tile],
                    swap_sem.at[n, 0],
                    {"row": r},
                )
        for c in col_peers:
            for b in range(blocks):
                send(
                    source.at[:, lanes(b * cols + c)],
                    by_col.at[n, row, col, :, b * tile : (b + 1) * tile],
                    swap_sem.at[n, 1],
                    {"col": c},
                )
    for n, source in enumerate(inputs):
        for h in range(halves):
            by_row[n, col, row, :, h * tile : (h + 1) * tile] = source[:, lanes(h * rows + row)]
        for b in range(blocks):
            by_col[n, row, col, :, b * tile : (b + 1) * tile] = source[:, lanes(b * cols + col)]

    def arrived(ref, sem):
        pltpu.make_async_copy(ref, ref, sem).wait()

    kinds = [(n, part) for n in range(2) for part in range(2)]
    axes = ("col", "row")
    held = (by_row, by_col)

    def piece(n, part, across, along, half=None):
        whole = held[part].at[n, place(axes[part], across, along)]
        if half is None:
            return whole
        size = whole.shape[0] // 2
        return whole.at[pl.ds(half * size, size)]

    def along_ring(n, part, across, along, way, half, sem):
        what = piece(n, part, across, along, half)
        where = {axes[part]: place(axes[part], 0, way)}
        send(what, what, ring_sem.at[n, part, sem], where)

    def to_core(n, part, across, along, half=None):
        if part == 1:
            what = piece(n, part, across, along, half)
            send(what, what, core_sem.at[n], {"row": row + 1 - 2 * core})

    def wait_ring(n, part, across, along, half, sem):
        arrived(piece(n, part, across, along, half), ring_sem.at[n, part, sem])

    for n, part in kinds:
        count = (rows if part == 0 else cols) - 1
        mine = (col if part == 0 else row,)
        arrived(held[part].at[n, mine[0], pl.ds(0, count)], swap_sem.at[n, part])
        along_ring(n, part, 0, 0, 1, None, 0)
        along_ring(n, part, 0, 0, -1, None, 1)
        what = piece(n, part, 0, 0)
        send(what, what, ring_sem.at[n, part, 2], {axes[part]: place(axes[part], 1, 0)})
        to_core(n, part, 0, 0)
    for n, part in kinds:
        wait_ring(n, part, 0, -1, None, 0)
        along_ring(n, part, 0, -1, 1, 0, 3)
        to_core(n, part, 0, -1)
        wait_ring(n, part, 0, 1, None, 1)
        along_ring(n, part, 0, 1, -1, 1, 4)
        to_core(n, part, 0, 1)
        wait_ring(n, part, 1, 0, None, 2)
        along_ring(n, part, 1, 0, 1, None, 5)
        along_ring(n, part, 1, 0, -1, None, 6)
        to_core(n, part, 1, 0)
    for n, part in kinds:
        wait_ring(n, part, 0, 2, 0, 3)
        to_core(n, part, 0, 2, 0)
        wait_ring(n, part, 0, 2, 1, 4)
        to_core(n, part, 0, 2, 1)
        wait_ring(n, part, 1, -1, None, 5)
        along_ring(n, part, 1, -1, 1, 0, 7)
        to_core(n, part, 1, -1)
        wait_ring(n, part, 1, 1, None, 6)
        along_ring(n, part, 1, 1, -1, 1, 8)
        to_core(n, part, 1, 1)
    for n, part in kinds:
        wait_ring(n, part, 1, 2, 0, 7)
        to_core(n, part, 1, 2, 0)
        wait_ring(n, part, 1, 2, 1, 8)
        to_core(n, part, 1, 2, 1)
    for n in range(2):
        arrived(by_col.at[n, pl.ds(0, rows // 2)], core_sem.at[n])

    total_a[...] = jnp.zeros_like(total_a)
    total_s[...] = jnp.zeros_like(total_s)

    def product(left, right):
        return lax.dot_general(
            left, right, (((0,), (0,)), ((), ())), preferred_element_type=jnp.float32
        )

    def add(c, carry):
        depth = rows * by_row.shape[3]
        psi_r = by_row[0, c].reshape(depth, halves * tile)
        hpsi_r = by_row[1, c].reshape(depth, halves * tile)
        psi_c = by_col[0, :, c].reshape(depth, blocks * tile)
        hpsi_c = by_col[1, :, c].reshape(depth, blocks * tile)
        total_a[...] += product(psi_r, hpsi_c) + product(hpsi_r, psi_c)
        total_s[...] += product(psi_r, psi_c)
        return carry

    lax.fori_loop(0, cols, add, 0)
    gvecs = rows * cols * by_row.shape[3]
    a_ref[...] = 0.5 * total_a[...]
    for b in range(blocks):
        corr_ref[pl.ds(b, halves * tile, stride=blocks), :] = total_s[
            :, b * tile : (b + 1) * tile
        ] * (1.0 / gvecs)

    def sent(ref):
        pltpu.make_async_copy(ref, ref, send_sem).wait()

    for n in range(2):
        sent(by_row.at[n, 0, pl.ds(0, rows - 1)])
        sent(by_col.at[n, 0, pl.ds(0, cols - 1)])
        for part in range(2):
            for _ in range(5):
                sent(held[part].at[n, 0])
            for _ in range(2):
                sent(held[part].at[n, 0])
        sent(by_col.at[n, pl.ds(0, rows // 2)])


def reduce_front(psi, hpsi, rows, cols, halves, blocks):
    tile = 128
    vmem = pl.BlockSpec(memory_space=pltpu.VMEM)
    height, width = halves * tile, blocks * tile
    return pl.pallas_call(
        front_kernel,
        out_shape=(
            jax.ShapeDtypeStruct((height, width), jnp.float32),
            jax.ShapeDtypeStruct((height * blocks, tile), jnp.float32),
        ),
        in_specs=[vmem, vmem],
        out_specs=(vmem, vmem),
        scratch_shapes=[
            pltpu.VMEM((2, cols, rows, psi.shape[0], height), psi.dtype),
            pltpu.VMEM((2, rows, cols, psi.shape[0], width), psi.dtype),
            pltpu.VMEM((height, width), jnp.float32),
            pltpu.VMEM((height, width), jnp.float32),
            pltpu.SemaphoreType.DMA,
            pltpu.SemaphoreType.DMA((2, 2)),
            pltpu.SemaphoreType.DMA((2, 2, 9)),
            pltpu.SemaphoreType.DMA((2,)),
        ],
        compiler_params=pltpu.CompilerParams(
            collective_id=1, has_side_effects=True, vmem_limit_bytes=48 * 1024 * 1024
        ),
        name="front",
    )(psi, hpsi)


def on_device(psi, hpsi, eigvec):
    row_tiles, _, tile_size, col_tiles = eigvec.shape[:4]
    row_count = lax.axis_size("row")
    col_count = lax.axis_size("col")
    reduced, correlation = reduce_front(psi, hpsi, row_count, col_count, row_tiles, col_tiles)
    updated, diagonal, offdiag, rotated = reduce_panel(
        reduced,
        psi,
        eigvec.reshape(row_tiles * tile_size, col_tiles * tile_size),
        row_count,
        col_count,
    )
    tile_shape = (row_tiles, 1, tile_size, col_tiles, 1, tile_size)
    return (
        correlation.reshape(tile_shape),
        updated.reshape(tile_shape),
        diagonal.reshape(PB),
        offdiag.reshape(PB),
        rotated.reshape(-1, col_tiles, 1, tile_size),
    )


def solution(mesh):
    return jax.shard_map(
        on_device,
        mesh=mesh,
        in_specs=(
            P(("row", "col"), None),
            P(("row", "col"), None),
            P(None, "row", None, None, "col", None),
        ),
        out_specs=(
            P(None, "row", None, None, "col", None),
            P(None, "row", None, None, "col", None),
            P(),
            P(),
            P("row", None, "col", None),
        ),
        check_vma=False,
    )
```

```python
import jax
import jax.numpy as jnp
from jax import lax
from jax.experimental import pallas as pl
from jax.experimental.pallas import tpu as pltpu
from jax.sharding import PartitionSpec as P

PB = 16
MESH = pl.DeviceIdType.MESH


def split_three(x):
    high = x.astype(jnp.bfloat16)
    rest = x - high.astype(jnp.float32)
    mid = rest.astype(jnp.bfloat16)
    low = (rest - mid.astype(jnp.float32)).astype(jnp.bfloat16)
    return high, mid, low


def lattice(row, col):
    pair = {"row": lax.div(row, 8), "col": lax.div(col, 4)}
    ring = {"row": lax.rem(lax.div(row, 2), 4), "col": lax.rem(col, 4)}
    return pair, ring


def whole_kernel(
    psi_ref,
    hpsi_ref,
    eig_ref,
    corr_ref,
    updated_ref,
    diag_ref,
    off_ref,
    rotated_ref,
    by_row,
    by_col,
    total_s,
    a_ref,
    psi_rows,
    eig_cols,
    rotated,
    rotated_tiles,
    a_plane,
    panel_in,
    panel,
    vecs,
    images,
    vec,
    lanes_sum,
    parts_out,
    parts_in,
    whole,
    send_sem,
    swap_sem,
    gather_sem,
    gather_core,
    ring_sem,
    panel_sem,
    parts_sem,
    eig_sem,
    core_sem,
    psi_sem,
):
    rows = lax.axis_size("row")
    cols = lax.axis_size("col")
    row = lax.axis_index("row")
    col = lax.axis_index("col")
    tile = 128
    height, width = a_ref.shape
    halves, blocks = height // tile, width // tile
    tiles = rows * halves
    turns = cols // 2
    pairs, rings = lattice(row, col)
    pair, ring = pairs["col"], rings["col"]
    inputs = (psi_ref, hpsi_ref)
    core = lax.rem(row, 2)

    def place(axis, across, along):
        p = lax.rem(pairs[axis] + across, 2)
        q = lax.rem(rings[axis] + along + 4, 4)
        return p * 8 + q * 2 + core if axis == "row" else p * 4 + q

    order = sorted(
        ((d, e) for d in range(rows) for e in range(2) if d + e > 0),
        key=lambda de: -min(de[0], rows - de[0]) - 4 * de[1],
    )
    peers = [
        {"row": lax.rem(row + d, rows), "col": lax.rem(pair + e, 2) * turns + ring}
        for d, e in order
    ]
    around = [{"row": row, "col": pair * turns + lax.rem(ring + d, turns)} for d in (1, 3, 2)]
    beyond = [
        {"row": row, "col": (1 - pair) * turns + lax.rem(ring + d, turns)} for d in (1, 3, 2)
    ]
    row_order = sorted(range(1, rows), key=lambda d: -min(d, rows - d))
    row_peers = [lax.rem(row + d, rows) for d in row_order]
    col_peers = [lax.rem(col + d, cols) for d in range(1, cols)]
    greeted = peers + around + beyond
    barrier = pltpu.get_barrier_semaphore()
    for peer in greeted:
        pl.semaphore_signal(barrier, inc=1, device_id=peer, device_id_type=MESH)
    pl.semaphore_wait(barrier, len(greeted))

    def send(source, target, sem, where):
        pltpu.make_async_remote_copy(
            src_ref=source,
            dst_ref=target,
            send_sem=send_sem,
            recv_sem=sem,
            device_id={"row": row, "col": col, **where},
            device_id_type=MESH,
        ).start()

    def lanes(tile_index):
        return pl.ds(pl.multiple_of(tile_index * tile, tile), tile)

    def arrived(ref, sem):
        pltpu.make_async_copy(ref, ref, sem).wait()

    for n, source in enumerate(inputs):
        for r in row_peers:
            for h in range(halves):
                send(
                    source.at[:, lanes(h * rows + r)],
                    by_row.at[n, col, row, :, h * tile : (h + 1) * tile],
                    swap_sem.at[n, 0],
                    {"row": r},
                )
        for c in col_peers:
            for b in range(blocks):
                send(
                    source.at[:, lanes(b * cols + c)],
                    by_col.at[n, row, col, :, b * tile : (b + 1) * tile],
                    swap_sem.at[n, 1],
                    {"col": c},
                )
    for n, source in enumerate(inputs):
        for h in range(halves):
            by_row[n, col, row, :, h * tile : (h + 1) * tile] = source[:, lanes(h * rows + row)]
        for b in range(blocks):
            by_col[n, row, col, :, b * tile : (b + 1) * tile] = source[:, lanes(b * cols + col)]

    kinds = [(n, part) for n in range(2) for part in range(2)]
    axes = ("col", "row")
    held = (by_row, by_col)

    def gathered(n, part, across, along, half=None):
        whole = held[part].at[n, place(axes[part], across, along)]
        if half is None:
            return whole
        size = whole.shape[0] // 2
        return whole.at[pl.ds(half * size, size)]

    def along_ring(n, part, across, along, way, half, sem):
        what = gathered(n, part, across, along, half)
        where = {axes[part]: place(axes[part], 0, way)}
        send(what, what, gather_sem.at[n, part, sem], where)

    def to_core(n, part, across, along, half=None):
        if part == 1:
            what = gathered(n, part, across, along, half)
            send(what, what, gather_core.at[n], {"row": row + 1 - 2 * core})

    def wait_ring(n, part, across, along, half, sem):
        arrived(gathered(n, part, across, along, half), gather_sem.at[n, part, sem])

    for n, part in kinds:
        count = (rows if part == 0 else cols) - 1
        mine = (col if part == 0 else row,)
        arrived(held[part].at[n, mine[0], pl.ds(0, count)], swap_sem.at[n, part])
        along_ring(n, part, 0, 0, 1, None, 0)
        along_ring(n, part, 0, 0, -1, None, 1)
        what = gathered(n, part, 0, 0)
        send(what, what, gather_sem.at[n, part, 2], {axes[part]: place(axes[part], 1, 0)})
        to_core(n, part, 0, 0)
    for n, part in kinds:
        wait_ring(n, part, 0, -1, None, 0)
        along_ring(n, part, 0, -1, 1, 0, 3)
        to_core(n, part, 0, -1)
        wait_ring(n, part, 0, 1, None, 1)
        along_ring(n, part, 0, 1, -1, 1, 4)
        to_core(n, part, 0, 1)
        wait_ring(n, part, 1, 0, None, 2)
        along_ring(n, part, 1, 0, 1, None, 5)
        along_ring(n, part, 1, 0, -1, None, 6)
        to_core(n, part, 1, 0)
    for n, part in kinds:
        wait_ring(n, part, 0, 2, 0, 3)
        to_core(n, part, 0, 2, 0)
        wait_ring(n, part, 0, 2, 1, 4)
        to_core(n, part, 0, 2, 1)
        wait_ring(n, part, 1, -1, None, 5)
        along_ring(n, part, 1, -1, 1, 0, 7)
        to_core(n, part, 1, -1)
        wait_ring(n, part, 1, 1, None, 6)
        along_ring(n, part, 1, 1, -1, 1, 8)
        to_core(n, part, 1, 1)
    for n, part in kinds:
        wait_ring(n, part, 1, 2, 0, 7)
        to_core(n, part, 1, 2, 0)
        wait_ring(n, part, 1, 2, 1, 8)
        to_core(n, part, 1, 2, 1)
    for n in range(2):
        arrived(by_col.at[n, pl.ds(0, rows // 2)], gather_core.at[n])


    def eig_place(across, along):
        return place("row", across, along)

    def psi_place(across, along):
        return place("col", across, along)

    def piece(held, index, half):
        whole = held.at[index]
        if half is None:
            return whole
        size = whole.shape[0] // 2
        return whole.at[pl.ds(half * size, size)]

    def eig_send(across, along, way, half, sem):
        what = piece(eig_cols, eig_place(across, along), half)
        to = eig_place(1, 0) if way is None else eig_place(0, way)
        send(what, what, eig_sem.at[sem], {"row": to, "col": col})

    def eig_core(across, along, half):
        what = piece(eig_cols, eig_place(across, along), half)
        send(what, what, core_sem, {"row": row + 1 - 2 * core, "col": col})

    def eig_wait(across, along, half, sem):
        arrived(piece(eig_cols, eig_place(across, along), half), eig_sem.at[sem])

    def psi_send(across, along, way, half, sem):
        what = piece(psi_rows, psi_place(across, along), half)
        to = psi_place(1, 0) if way is None else psi_place(0, way)
        send(what, what, psi_sem.at[sem], {"row": row, "col": to})

    def psi_wait(across, along, half, sem):
        arrived(piece(psi_rows, psi_place(across, along), half), psi_sem.at[sem])

    eig_cols[row] = eig_ref[...]
    psi_rows[col] = psi_ref[...]
    eig_send(0, 0, 1, None, 0)
    eig_send(0, 0, -1, None, 1)
    eig_send(0, 0, None, None, 2)
    eig_core(0, 0, None)
    psi_send(0, 0, None, None, 2)


    depth = rows * by_row.shape[3]

    def row_block(n, c):
        return by_row[n, c].reshape(depth, halves * tile)

    def col_block(n, c):
        return by_col[n, :, c].reshape(depth, blocks * tile)

    def product(left, right):
        return lax.dot_general(
            left, right, (((0,), (0,)), ((), ())), preferred_element_type=jnp.float32
        )

    def add_s(c, carry):
        total_s[...] += product(row_block(0, c), col_block(0, c))
        return carry

    def add_a(c, carry):
        a_ref[...] += product(row_block(0, c), col_block(1, c)) + product(
            row_block(1, c), col_block(0, c)
        )
        return carry

    a_ref[...] = jnp.zeros_like(a_ref)
    lax.fori_loop(0, cols, add_a, 0)
    a_ref[...] = 0.5 * a_ref[...]

    def to_peers(source, target, recv):
        for peer in peers:
            send(source, target, recv, peer)

    @pl.when(col == 0)
    def _():
        for half in range(halves):
            first = a_ref[half * tile : (half + 1) * tile, 0:tile]
            panel_in[row, :, half, :] = jnp.transpose(first)[0:PB, :]
        for peer in around:
            send(panel_in.at[row], panel_in.at[row], panel_sem.at[0], peer)

    above, below = lax.rem(ring + 1, turns), lax.rem(ring + turns - 1, turns)
    half_rows = height // 2

    def part_of(where, half):
        return a_plane.at[where, pl.ds(half * half_rows, half_rows)]

    for half in range(2):
        for way, part in ((0, half), (1, 1 - half)):
            send(
                a_ref.at[pl.ds(part * half_rows, half_rows)],
                part_of(ring, part),
                ring_sem.at[2 * way + part],
                around[way],
            )


    @pl.when((pair == 0) & (ring > 0))
    def _():
        arrived(panel_in.at[row], panel_sem.at[0])

    @pl.when(pair == 0)
    def _():
        to_peers(panel_in.at[row], panel_in.at[row], panel_sem.at[1])

    a_plane[ring] = a_ref[...]
    vecs[...] = jnp.zeros_like(vecs)
    images[...] = jnp.zeros_like(images)
    spot = lax.broadcasted_iota(jnp.int32, (tiles, tile), 0)
    lane = lax.broadcasted_iota(jnp.int32, (tiles, tile), 1)
    positions = ((spot % halves) * rows + spot // halves) * tile + lane
    slot = lax.broadcasted_iota(jnp.int32, (8, tile), 1)

    @pl.when(pair == 0)
    def _():
        arrived(panel_in.at[pl.ds(0, rows - 1)], panel_sem.at[1])

    @pl.when(pair > 0)
    def _():
        arrived(panel_in, panel_sem.at[1])

    for r in range(rows):
        panel[:, r * halves : (r + 1) * halves, :] = panel_in[r]
    arrived(part_of(below, 0), ring_sem.at[0])
    send(part_of(below, 0), part_of(below, 0), ring_sem.at[4], around[0])
    arrived(part_of(above, 1), ring_sem.at[3])
    send(part_of(above, 1), part_of(above, 1), ring_sem.at[5], around[1])
    eig_wait(0, -1, None, 0)
    eig_send(0, -1, 1, 0, 3)
    eig_core(0, -1, None)
    eig_wait(0, 1, None, 1)
    eig_send(0, 1, -1, 1, 4)
    eig_core(0, 1, None)
    eig_wait(1, 0, None, 2)
    eig_send(1, 0, 1, None, 5)
    eig_send(1, 0, -1, None, 6)
    eig_core(1, 0, None)
    psi_send(0, 0, 1, None, 0)
    psi_send(0, 0, -1, None, 1)
    psi_wait(1, 0, None, 2)
    psi_send(1, 0, 1, None, 5)
    psi_send(1, 0, -1, None, 6)
    across = lax.rem(ring + 2, turns)
    arrived(part_of(below, 1), ring_sem.at[1])
    arrived(part_of(above, 0), ring_sem.at[2])
    arrived(part_of(across, 0), ring_sem.at[4])
    arrived(part_of(across, 1), ring_sem.at[5])

    def background(step):
        @pl.when(step == 0)
        def _():
            eig_wait(0, 2, 0, 3)
            eig_core(0, 2, 0)
            eig_wait(0, 2, 1, 4)
            eig_core(0, 2, 1)
            eig_wait(1, -1, None, 5)
            eig_send(1, -1, 1, 0, 7)
            eig_core(1, -1, None)
            eig_wait(1, 1, None, 6)
            eig_send(1, 1, -1, 1, 8)
            eig_core(1, 1, None)

        @pl.when(step == 2)
        def _():
            eig_wait(1, 2, 0, 7)
            eig_core(1, 2, 0)
            eig_wait(1, 2, 1, 8)
            eig_core(1, 2, 1)
            psi_wait(0, -1, None, 0)
            psi_send(0, -1, 1, 0, 3)
            psi_wait(0, 1, None, 1)
            psi_send(0, 1, -1, 1, 4)

        @pl.when(step == 3)
        def _():
            total_s[...] = jnp.zeros_like(total_s)
            lax.fori_loop(0, cols, add_s, 0)

        @pl.when(step == 5)
        def _():
            scale = 1.0 / (rows * cols * psi_ref.shape[0])
            for b in range(blocks):
                corr_ref[pl.ds(b, height, stride=blocks), :] = scale * total_s[
                    :, b * tile : (b + 1) * tile
                ]

        @pl.when(step == 4)
        def _():
            psi_wait(1, -1, None, 5)
            psi_send(1, -1, 1, 0, 7)
            psi_wait(1, 1, None, 6)
            psi_send(1, 1, -1, 1, 8)

        @pl.when(step == 6)
        def _():
            for half in range(2):
                psi_wait(0, 2, half, 3 + half)
                psi_wait(1, 2, half, 7 + half)
            arrived(eig_cols.at[pl.ds(0, rows // 2)], core_sem)
            rotated[...] = jnp.zeros_like(rotated)

        @pl.when((step >= PB // 2 - 1) & (step < PB - 1))
        def _():
            per = rows // (PB // 2)
            for k in range(per):
                r = (step - PB // 2 + 1) * per + k
                left = [
                    psi_rows[:, :, pl.ds(pl.multiple_of((h * rows + r) * tile, tile), tile)]
                    for h in range(halves)
                ]
                left = jnp.concatenate([x.reshape(-1, tile) for x in left], axis=1)
                rotated[...] += jnp.dot(left, eig_cols[r], preferred_element_type=jnp.float32)

        @pl.when(step == PB - 1)
        def _():
            depth = rotated.shape[0]
            for b in range(blocks):
                rotated_tiles[pl.ds(b, depth, stride=blocks), :] = rotated[
                    :, b * tile : (b + 1) * tile
                ]
            rotated_ref[...] = rotated_tiles[...].astype(rotated_ref.dtype)

    def total(x):
        return jnp.sum(x, axis=(0, 1), keepdims=True)

    def totals(x):
        return jnp.sum(x, axis=(1, 2), keepdims=True)

    def reflector(column, step):
        at = total(jnp.where(positions == step, column, 0.0))
        pivot = total(jnp.where(positions == step + 1, column, 0.0))
        under = positions > step + 1
        tail = total(jnp.where(under, column * column, 0.0))
        length = jnp.sqrt(pivot * pivot + tail)
        beta = jnp.where(pivot >= 0.0, -length, length)
        tau = (beta - pivot) / beta
        scale = 1.0 / (pivot - beta)
        vector = jnp.where(positions == step + 1, 1.0, jnp.where(under, column * scale, 0.0))
        return at, beta, tau, vector

    def advance(step, carry):
        column, diagonal, offdiag = carry
        at, beta, tau, vector = reflector(column, step)
        diagonal = jnp.where(slot == step, at, diagonal)
        offdiag = jnp.where(slot == step, beta, offdiag)
        vec[...] = vector
        spread = []
        for y in range(turns):
            for b in range(blocks):
                t = b * cols + pair * turns + y
                e = lax.rem(t, rows) * halves + lax.div(t, rows)
                spread.append(jnp.broadcast_to(vec[pl.ds(e, 1), :], (8, tile)))

        def band(group, _):
            at_rows = pl.ds(pl.multiple_of(group * 8, 8), 8)
            sums = [jnp.zeros((8, tile), jnp.float32) for _ in range(4)]
            for y in range(turns):
                for b in range(blocks):
                    block = a_plane[y, at_rows, b * tile : (b + 1) * tile]
                    sums[b] = sums[b] + block * spread[y * blocks + b]
            lanes_sum[at_rows, :] = (sums[0] + sums[1]) + (sums[2] + sums[3])
            return 0

        lax.fori_loop(0, height // 8, band, 0, unroll=4)
        ones = jnp.ones((16, tile), jnp.bfloat16)
        product = jnp.zeros((16, height), jnp.float32)
        for piece in split_three(lanes_sum[...]):
            product = product + lax.dot_general(
                ones, piece, (((1,), (1,)), ((), ())), preferred_element_type=jnp.float32
            )
        for half in range(halves):
            parts_out[step, half : half + 1, :] = product[0:1, half * tile : (half + 1) * tile]
        to_peers(parts_out.at[step], parts_in.at[step, pair * rows + row], parts_sem.at[step])
        parts_in[step, pair * rows + row] = parts_out[step]
        background(step)
        by_vecs = totals(vecs[...] * vector[None])
        by_images = totals(images[...] * vector[None])
        known = jnp.sum(vecs[...] * by_images + images[...] * by_vecs, axis=0)
        following = jnp.minimum(step + 1, PB - 1)
        here = positions == following
        head_v = totals(jnp.where(here[None], vecs[...], 0.0))
        head_w = totals(jnp.where(here[None], images[...], 0.0))
        ahead = panel[following] - jnp.sum(vecs[...] * head_w + images[...] * head_v, axis=0)
        vecs[step] = vector
        lead_v = total(jnp.where(here, vector, 0.0))
        half_tau = 0.5 * tau * tau
        arrived(parts_in.at[step, pl.ds(0, 2 * rows - 1)], parts_sem.at[step])
        for r in range(rows):
            whole[r * halves : (r + 1) * halves, :] = parts_in[step, r] + parts_in[step, rows + r]
        change = whole[...] - known
        along = half_tau * total(change * vector)
        lead_w = tau * total(jnp.where(here, change, 0.0)) - along * lead_v
        image = tau * change - along * vector
        images[step] = image
        column = ahead - vector * lead_w - image * lead_v
        return column, diagonal, offdiag

    nothing = jnp.zeros((8, tile), jnp.float32)
    _, diagonal, offdiag = lax.fori_loop(0, PB, advance, (panel[0], nothing, nothing))
    diag_ref[...] = diagonal[0:1, 0:PB]
    off_ref[...] = offdiag[0:1, 0:PB]
    left_v = [vecs[:, pl.ds(halves * row + h, 1), :].reshape(PB, tile) for h in range(halves)]
    left_w = [images[:, pl.ds(halves * row + h, 1), :].reshape(PB, tile) for h in range(halves)]
    for b in range(blocks):
        t = b * cols + col
        e = (t % rows) * halves + t // rows
        right_v = vecs[:, pl.ds(e, 1), :].reshape(PB, tile)
        right_w = images[:, pl.ds(e, 1), :].reshape(PB, tile)
        for h in range(halves):
            change = lax.dot_general(
                jnp.concatenate([left_v[h], left_w[h]], axis=0),
                jnp.concatenate([right_w, right_v], axis=0),
                (((0,), (0,)), ((), ())),
                precision=lax.Precision.HIGHEST,
                preferred_element_type=jnp.float32,
            )
            block = a_ref[h * tile : (h + 1) * tile, b * tile : (b + 1) * tile]
            updated_ref[pl.ds(h * tile * blocks + b, tile, stride=blocks), :] = block - change


    def sent(ref):
        pltpu.make_async_copy(ref, ref, send_sem).wait()

    @pl.when(col == 0)
    def _():
        sent(panel_in.at[pl.ds(0, len(around))])

    @pl.when(pair == 0)
    def _():
        sent(panel_in.at[pl.ds(0, rows)])
        sent(panel_in.at[pl.ds(0, rows - 1)])

    for _ in range(3):
        sent(a_ref)
    sent(eig_cols.at[pl.ds(0, 7)])
    sent(eig_cols.at[pl.ds(0, rows // 2)])
    sent(psi_rows.at[pl.ds(0, 7)])

    def drain(step, carry):
        sent(parts_in.at[step, pl.ds(0, 2 * rows - 1)])
        return carry

    lax.fori_loop(0, PB, drain, 0)

    for n in range(2):
        sent(by_row.at[n, 0, pl.ds(0, rows - 1)])
        sent(by_col.at[n, 0, pl.ds(0, cols - 1)])
        sent(by_row.at[n, pl.ds(0, 7)])
        sent(by_col.at[n, pl.ds(0, 7)])
        sent(by_col.at[n, pl.ds(0, rows // 2)])


def reduce_and_rotate(psi, hpsi, eigvec, rows, cols):
    height, width = eigvec.shape
    tile = 128
    halves = height // tile
    tiles = rows * halves
    depth = cols * psi.shape[0]
    vmem = pl.BlockSpec(memory_space=pltpu.VMEM)
    block = pltpu.VMEM((height, width), jnp.float32)
    vectors = pltpu.VMEM((PB, tiles, tile), jnp.float32)
    laid = jax.ShapeDtypeStruct((height * width // tile, tile), jnp.float32)
    return pl.pallas_call(
        whole_kernel,
        out_shape=(
            laid,
            laid,
            jax.ShapeDtypeStruct((1, PB), jnp.float32),
            jax.ShapeDtypeStruct((1, PB), jnp.float32),
            jax.ShapeDtypeStruct((depth * width // tile, tile), psi.dtype),
        ),
        in_specs=[vmem] * 3,
        out_specs=(vmem,) * 5,
        scratch_shapes=[
            pltpu.VMEM((2, cols, rows, psi.shape[0], height), psi.dtype),
            pltpu.VMEM((2, rows, cols, psi.shape[0], width), psi.dtype),
            block,
            block,
            pltpu.VMEM((cols, *psi.shape), psi.dtype),
            pltpu.VMEM((rows, *eigvec.shape), eigvec.dtype),
            pltpu.VMEM((depth, width), jnp.float32),
            pltpu.VMEM((depth * width // tile, tile), jnp.float32),
            pltpu.VMEM((cols // 2, height, width), jnp.float32),
            pltpu.VMEM((rows, PB, halves, tile), jnp.float32),
            vectors,
            vectors,
            vectors,
            pltpu.VMEM((tiles, tile), jnp.float32),
            pltpu.VMEM((height, tile), jnp.float32),
            pltpu.VMEM((PB, halves, tile), jnp.float32),
            pltpu.VMEM((PB, 2 * rows, halves, tile), jnp.float32),
            pltpu.VMEM((tiles, tile), jnp.float32),
            pltpu.SemaphoreType.DMA,
            pltpu.SemaphoreType.DMA((2, 2)),
            pltpu.SemaphoreType.DMA((2, 2, 9)),
            pltpu.SemaphoreType.DMA((2,)),
            pltpu.SemaphoreType.DMA((6,)),
            pltpu.SemaphoreType.DMA((2,)),
            pltpu.SemaphoreType.DMA((PB,)),
            pltpu.SemaphoreType.DMA((9,)),
            pltpu.SemaphoreType.DMA,
            pltpu.SemaphoreType.DMA((9,)),
        ],
        compiler_params=pltpu.CompilerParams(
            collective_id=0, has_side_effects=True, vmem_limit_bytes=56 * 1024 * 1024
        ),
        name="whole",
    )(psi, hpsi, eigvec)


def on_device(psi, hpsi, eigvec):
    row_tiles, _, tile_size, col_tiles = eigvec.shape[:4]
    correlation, updated, diagonal, offdiag, rotated = reduce_and_rotate(
        psi,
        hpsi,
        eigvec.reshape(row_tiles * tile_size, col_tiles * tile_size),
        lax.axis_size("row"),
        lax.axis_size("col"),
    )
    tile_shape = (row_tiles, 1, tile_size, col_tiles, 1, tile_size)
    return (
        correlation.reshape(tile_shape),
        updated.reshape(tile_shape),
        diagonal.reshape(PB),
        offdiag.reshape(PB),
        rotated.reshape(-1, col_tiles, 1, tile_size),
    )


def solution(mesh):
    return jax.shard_map(
        on_device,
        mesh=mesh,
        in_specs=(
            P(("row", "col"), None),
            P(("row", "col"), None),
            P(None, "row", None, None, "col", None),
        ),
        out_specs=(
            P(None, "row", None, None, "col", None),
            P(None, "row", None, None, "col", None),
            P(),
            P(),
            P("row", None, "col", None),
        ),
        check_vma=False,
    )
```

```python
import jax
import jax.numpy as jnp
from jax import lax
from jax.experimental import pallas as pl
from jax.experimental.pallas import tpu as pltpu
from jax.sharding import PartitionSpec as P

PB = 16
MESH = pl.DeviceIdType.MESH


def split_three(x):
    high = x.astype(jnp.bfloat16)
    rest = x - high.astype(jnp.float32)
    mid = rest.astype(jnp.bfloat16)
    low = (rest - mid.astype(jnp.float32)).astype(jnp.bfloat16)
    return high, mid, low


def lattice(row, col):
    pair = {"row": lax.div(row, 8), "col": lax.div(col, 4)}
    ring = {"row": lax.rem(lax.div(row, 2), 4), "col": lax.rem(col, 4)}
    return pair, ring


def whole_kernel(
    psi_ref,
    hpsi_ref,
    eig_ref,
    corr_ref,
    updated_ref,
    diag_ref,
    off_ref,
    rotated_ref,
    by_row,
    by_col,
    total_s,
    a_ref,
    psi_rows,
    eig_cols,
    rotated,
    rotated_tiles,
    a_plane,
    panel_in,
    panel,
    vecs,
    images,
    vec,
    lanes_sum,
    parts_out,
    parts_in,
    whole,
    send_sem,
    swap_sem,
    gather_sem,
    gather_core,
    ring_sem,
    panel_sem,
    parts_sem,
    eig_sem,
    core_sem,
    psi_sem,
):
    rows = lax.axis_size("row")
    cols = lax.axis_size("col")
    row = lax.axis_index("row")
    col = lax.axis_index("col")
    tile = 128
    height, width = a_ref.shape
    halves, blocks = height // tile, width // tile
    tiles = rows * halves
    turns = cols // 2
    pairs, rings = lattice(row, col)
    pair, ring = pairs["col"], rings["col"]
    inputs = (psi_ref, hpsi_ref)
    core = lax.rem(row, 2)

    def place(axis, across, along):
        p = lax.rem(pairs[axis] + across, 2)
        q = lax.rem(rings[axis] + along + 4, 4)
        return p * 8 + q * 2 + core if axis == "row" else p * 4 + q

    order = sorted(
        ((d, e) for d in range(rows) for e in range(2) if d + e > 0),
        key=lambda de: -min(de[0], rows - de[0]) - 4 * de[1],
    )
    peers = [
        {"row": lax.rem(row + d, rows), "col": lax.rem(pair + e, 2) * turns + ring}
        for d, e in order
    ]
    around = [{"row": row, "col": pair * turns + lax.rem(ring + d, turns)} for d in (1, 3, 2)]
    beyond = [
        {"row": row, "col": (1 - pair) * turns + lax.rem(ring + d, turns)} for d in (1, 3, 2)
    ]
    row_order = sorted(range(1, rows), key=lambda d: -min(d, rows - d))
    row_peers = [lax.rem(row + d, rows) for d in row_order]
    col_peers = [lax.rem(col + d, cols) for d in range(1, cols)]
    greeted = peers + around + beyond
    barrier = pltpu.get_barrier_semaphore()
    for peer in greeted:
        pl.semaphore_signal(barrier, inc=1, device_id=peer, device_id_type=MESH)
    pl.semaphore_wait(barrier, len(greeted))

    def send(source, target, sem, where):
        pltpu.make_async_remote_copy(
            src_ref=source,
            dst_ref=target,
            send_sem=send_sem,
            recv_sem=sem,
            device_id={"row": row, "col": col, **where},
            device_id_type=MESH,
        ).start()

    def lanes(tile_index):
        return pl.ds(pl.multiple_of(tile_index * tile, tile), tile)

    def arrived(ref, sem):
        pltpu.make_async_copy(ref, ref, sem).wait()

    for n, source in enumerate(inputs):
        for r in row_peers:
            for h in range(halves):
                send(
                    source.at[:, lanes(h * rows + r)],
                    by_row.at[n, col, row, :, h * tile : (h + 1) * tile],
                    swap_sem.at[n, 0],
                    {"row": r},
                )
        for c in col_peers:
            for b in range(blocks):
                send(
                    source.at[:, lanes(b * cols + c)],
                    by_col.at[n, row, col, :, b * tile : (b + 1) * tile],
                    swap_sem.at[n, 1],
                    {"col": c},
                )
    for n, source in enumerate(inputs):
        for h in range(halves):
            by_row[n, col, row, :, h * tile : (h + 1) * tile] = source[:, lanes(h * rows + row)]
        for b in range(blocks):
            by_col[n, row, col, :, b * tile : (b + 1) * tile] = source[:, lanes(b * cols + col)]

    kinds = [(n, part) for n in range(2) for part in range(2)]
    axes = ("col", "row")
    held = (by_row, by_col)

    def gathered(n, part, across, along, half=None):
        whole = held[part].at[n, place(axes[part], across, along)]
        if half is None:
            return whole
        size = whole.shape[0] // 2
        return whole.at[pl.ds(half * size, size)]

    def along_ring(n, part, across, along, way, half, sem):
        what = gathered(n, part, across, along, half)
        where = {axes[part]: place(axes[part], 0, way)}
        send(what, what, gather_sem.at[n, part, sem], where)

    def to_core(n, part, across, along, half=None):
        if part == 1:
            what = gathered(n, part, across, along, half)
            send(what, what, gather_core.at[n], {"row": row + 1 - 2 * core})

    def wait_ring(n, part, across, along, half, sem):
        arrived(gathered(n, part, across, along, half), gather_sem.at[n, part, sem])

    for n, part in kinds:
        count = (rows if part == 0 else cols) - 1
        mine = (col if part == 0 else row,)
        arrived(held[part].at[n, mine[0], pl.ds(0, count)], swap_sem.at[n, part])
        along_ring(n, part, 0, 0, 1, None, 0)
        along_ring(n, part, 0, 0, -1, None, 1)
        what = gathered(n, part, 0, 0)
        send(what, what, gather_sem.at[n, part, 2], {axes[part]: place(axes[part], 1, 0)})
        to_core(n, part, 0, 0)
    for n, part in kinds:
        wait_ring(n, part, 0, -1, None, 0)
        along_ring(n, part, 0, -1, 1, 0, 3)
        to_core(n, part, 0, -1)
        wait_ring(n, part, 0, 1, None, 1)
        along_ring(n, part, 0, 1, -1, 1, 4)
        to_core(n, part, 0, 1)
        wait_ring(n, part, 1, 0, None, 2)
        along_ring(n, part, 1, 0, 1, None, 5)
        along_ring(n, part, 1, 0, -1, None, 6)
        to_core(n, part, 1, 0)
    for n, part in kinds:
        wait_ring(n, part, 0, 2, 0, 3)
        to_core(n, part, 0, 2, 0)
        wait_ring(n, part, 0, 2, 1, 4)
        to_core(n, part, 0, 2, 1)
        wait_ring(n, part, 1, -1, None, 5)
        along_ring(n, part, 1, -1, 1, 0, 7)
        to_core(n, part, 1, -1)
        wait_ring(n, part, 1, 1, None, 6)
        along_ring(n, part, 1, 1, -1, 1, 8)
        to_core(n, part, 1, 1)
    for n, part in kinds:
        wait_ring(n, part, 1, 2, 0, 7)
        to_core(n, part, 1, 2, 0)
        wait_ring(n, part, 1, 2, 1, 8)
        to_core(n, part, 1, 2, 1)
    for n in range(2):
        arrived(by_col.at[n, pl.ds(0, rows // 2)], gather_core.at[n])


    def eig_place(across, along):
        return place("row", across, along)

    def psi_place(across, along):
        return place("col", across, along)

    def piece(held, index, half):
        whole = held.at[index]
        if half is None:
            return whole
        size = whole.shape[0] // 2
        return whole.at[pl.ds(half * size, size)]

    def eig_send(across, along, way, half, sem):
        what = piece(eig_cols, eig_place(across, along), half)
        to = eig_place(1, 0) if way is None else eig_place(0, way)
        send(what, what, eig_sem.at[sem], {"row": to, "col": col})

    def eig_core(across, along, half):
        what = piece(eig_cols, eig_place(across, along), half)
        send(what, what, core_sem, {"row": row + 1 - 2 * core, "col": col})

    def eig_wait(across, along, half, sem):
        arrived(piece(eig_cols, eig_place(across, along), half), eig_sem.at[sem])

    def psi_send(across, along, way, half, sem):
        what = piece(psi_rows, psi_place(across, along), half)
        to = psi_place(1, 0) if way is None else psi_place(0, way)
        send(what, what, psi_sem.at[sem], {"row": row, "col": to})

    def psi_wait(across, along, half, sem):
        arrived(piece(psi_rows, psi_place(across, along), half), psi_sem.at[sem])

    depth = rows * by_row.shape[3]

    def row_block(n, c):
        return by_row[n, c].reshape(depth, halves * tile)

    def col_block(n, c):
        return by_col[n, :, c].reshape(depth, blocks * tile)

    def product(left, right):
        return lax.dot_general(
            left, right, (((0,), (0,)), ((), ())), preferred_element_type=jnp.float32
        )

    def add_s(c, carry):
        total_s[...] += product(row_block(0, c), col_block(0, c))
        return carry

    def add_a(c, carry):
        a_ref[...] += product(row_block(0, c), col_block(1, c)) + product(
            row_block(1, c), col_block(0, c)
        )
        return carry

    a_ref[...] = jnp.zeros_like(a_ref)
    lax.fori_loop(0, cols, add_a, 0)
    a_ref[...] = 0.5 * a_ref[...]

    def to_peers(source, target, recv):
        for peer in peers:
            send(source, target, recv, peer)

    @pl.when(col == 0)
    def _():
        for half in range(halves):
            first = a_ref[half * tile : (half + 1) * tile, 0:tile]
            panel_in[row, :, half, :] = jnp.transpose(first)[0:PB, :]
        for peer in around:
            send(panel_in.at[row], panel_in.at[row], panel_sem.at[0], peer)

    above, below = lax.rem(ring + 1, turns), lax.rem(ring + turns - 1, turns)
    half_rows = height // 2

    def part_of(where, half):
        return a_plane.at[where, pl.ds(half * half_rows, half_rows)]

    for half in range(2):
        for way, part in ((0, half), (1, 1 - half)):
            send(
                a_ref.at[pl.ds(part * half_rows, half_rows)],
                part_of(ring, part),
                ring_sem.at[2 * way + part],
                around[way],
            )


    @pl.when((pair == 0) & (ring > 0))
    def _():
        arrived(panel_in.at[row], panel_sem.at[0])

    @pl.when(pair == 0)
    def _():
        to_peers(panel_in.at[row], panel_in.at[row], panel_sem.at[1])

    eig_cols[row] = eig_ref[...]
    psi_rows[col] = psi_ref[...]
    eig_send(0, 0, 1, None, 0)
    eig_send(0, 0, -1, None, 1)
    eig_send(0, 0, None, None, 2)
    eig_core(0, 0, None)
    psi_send(0, 0, None, None, 2)


    a_plane[ring] = a_ref[...]
    vecs[...] = jnp.zeros_like(vecs)
    images[...] = jnp.zeros_like(images)
    spot = lax.broadcasted_iota(jnp.int32, (tiles, tile), 0)
    lane = lax.broadcasted_iota(jnp.int32, (tiles, tile), 1)
    positions = ((spot % halves) * rows + spot // halves) * tile + lane
    slot = lax.broadcasted_iota(jnp.int32, (8, tile), 1)

    @pl.when(pair == 0)
    def _():
        arrived(panel_in.at[pl.ds(0, rows - 1)], panel_sem.at[1])

    @pl.when(pair > 0)
    def _():
        arrived(panel_in, panel_sem.at[1])

    for r in range(rows):
        panel[:, r * halves : (r + 1) * halves, :] = panel_in[r]
    arrived(part_of(below, 0), ring_sem.at[0])
    send(part_of(below, 0), part_of(below, 0), ring_sem.at[4], around[0])
    arrived(part_of(above, 1), ring_sem.at[3])
    send(part_of(above, 1), part_of(above, 1), ring_sem.at[5], around[1])
    eig_wait(0, -1, None, 0)
    eig_send(0, -1, 1, 0, 3)
    eig_core(0, -1, None)
    eig_wait(0, 1, None, 1)
    eig_send(0, 1, -1, 1, 4)
    eig_core(0, 1, None)
    eig_wait(1, 0, None, 2)
    eig_send(1, 0, 1, None, 5)
    eig_send(1, 0, -1, None, 6)
    eig_core(1, 0, None)
    psi_send(0, 0, 1, None, 0)
    psi_send(0, 0, -1, None, 1)
    psi_wait(1, 0, None, 2)
    psi_send(1, 0, 1, None, 5)
    psi_send(1, 0, -1, None, 6)
    across = lax.rem(ring + 2, turns)
    arrived(part_of(below, 1), ring_sem.at[1])
    arrived(part_of(above, 0), ring_sem.at[2])
    arrived(part_of(across, 0), ring_sem.at[4])
    arrived(part_of(across, 1), ring_sem.at[5])

    def background(step):
        @pl.when(step == 0)
        def _():
            eig_wait(0, 2, 0, 3)
            eig_core(0, 2, 0)
            eig_wait(0, 2, 1, 4)
            eig_core(0, 2, 1)
            eig_wait(1, -1, None, 5)
            eig_send(1, -1, 1, 0, 7)
            eig_core(1, -1, None)
            eig_wait(1, 1, None, 6)
            eig_send(1, 1, -1, 1, 8)
            eig_core(1, 1, None)

        @pl.when(step == 2)
        def _():
            eig_wait(1, 2, 0, 7)
            eig_core(1, 2, 0)
            eig_wait(1, 2, 1, 8)
            eig_core(1, 2, 1)
            psi_wait(0, -1, None, 0)
            psi_send(0, -1, 1, 0, 3)
            psi_wait(0, 1, None, 1)
            psi_send(0, 1, -1, 1, 4)

        @pl.when(step == 3)
        def _():
            total_s[...] = jnp.zeros_like(total_s)
            lax.fori_loop(0, cols, add_s, 0)

        @pl.when(step == 5)
        def _():
            scale = 1.0 / (rows * cols * psi_ref.shape[0])
            for b in range(blocks):
                corr_ref[pl.ds(b, height, stride=blocks), :] = scale * total_s[
                    :, b * tile : (b + 1) * tile
                ]

        @pl.when(step == 4)
        def _():
            psi_wait(1, -1, None, 5)
            psi_send(1, -1, 1, 0, 7)
            psi_wait(1, 1, None, 6)
            psi_send(1, 1, -1, 1, 8)

        @pl.when(step == 6)
        def _():
            for half in range(2):
                psi_wait(0, 2, half, 3 + half)
                psi_wait(1, 2, half, 7 + half)
            arrived(eig_cols.at[pl.ds(0, rows // 2)], core_sem)
            rotated[...] = jnp.zeros_like(rotated)

        @pl.when((step >= PB // 2 - 1) & (step < PB - 1))
        def _():
            per = rows // (PB // 2)
            for k in range(per):
                r = (step - PB // 2 + 1) * per + k
                left = [
                    psi_rows[:, :, pl.ds(pl.multiple_of((h * rows + r) * tile, tile), tile)]
                    for h in range(halves)
                ]
                left = jnp.concatenate([x.reshape(-1, tile) for x in left], axis=1)
                rotated[...] += jnp.dot(left, eig_cols[r], preferred_element_type=jnp.float32)

        @pl.when(step == PB - 1)
        def _():
            depth = rotated.shape[0]
            for b in range(blocks):
                rotated_tiles[pl.ds(b, depth, stride=blocks), :] = rotated[
                    :, b * tile : (b + 1) * tile
                ]
            rotated_ref[...] = rotated_tiles[...].astype(rotated_ref.dtype)

    def total(x):
        return jnp.sum(x, axis=(0, 1), keepdims=True)

    def totals(x):
        return jnp.sum(x, axis=(1, 2), keepdims=True)

    def reflector(column, step):
        at = total(jnp.where(positions == step, column, 0.0))
        pivot = total(jnp.where(positions == step + 1, column, 0.0))
        under = positions > step + 1
        tail = total(jnp.where(under, column * column, 0.0))
        length = jnp.sqrt(pivot * pivot + tail)
        beta = jnp.where(pivot >= 0.0, -length, length)
        tau = (beta - pivot) / beta
        scale = 1.0 / (pivot - beta)
        vector = jnp.where(positions == step + 1, 1.0, jnp.where(under, column * scale, 0.0))
        return at, beta, tau, vector

    def advance(step, carry):
        column, diagonal, offdiag = carry
        at, beta, tau, vector = reflector(column, step)
        diagonal = jnp.where(slot == step, at, diagonal)
        offdiag = jnp.where(slot == step, beta, offdiag)
        vec[...] = vector
        spread = []
        for y in range(turns):
            for b in range(blocks):
                t = b * cols + pair * turns + y
                e = lax.rem(t, rows) * halves + lax.div(t, rows)
                spread.append(jnp.broadcast_to(vec[pl.ds(e, 1), :], (8, tile)))

        def band(group, _):
            at_rows = pl.ds(pl.multiple_of(group * 8, 8), 8)
            sums = [jnp.zeros((8, tile), jnp.float32) for _ in range(4)]
            for y in range(turns):
                for b in range(blocks):
                    block = a_plane[y, at_rows, b * tile : (b + 1) * tile]
                    sums[b] = sums[b] + block * spread[y * blocks + b]
            lanes_sum[at_rows, :] = (sums[0] + sums[1]) + (sums[2] + sums[3])
            return 0

        lax.fori_loop(0, height // 8, band, 0, unroll=4)
        ones = jnp.ones((16, tile), jnp.bfloat16)
        product = jnp.zeros((16, height), jnp.float32)
        for piece in split_three(lanes_sum[...]):
            product = product + lax.dot_general(
                ones, piece, (((1,), (1,)), ((), ())), preferred_element_type=jnp.float32
            )
        for half in range(halves):
            parts_out[step, half : half + 1, :] = product[0:1, half * tile : (half + 1) * tile]
        to_peers(parts_out.at[step], parts_in.at[step, pair * rows + row], parts_sem.at[step])
        parts_in[step, pair * rows + row] = parts_out[step]
        background(step)
        by_vecs = totals(vecs[...] * vector[None])
        by_images = totals(images[...] * vector[None])
        known = jnp.sum(vecs[...] * by_images + images[...] * by_vecs, axis=0)
        following = jnp.minimum(step + 1, PB - 1)
        here = positions == following
        head_v = totals(jnp.where(here[None], vecs[...], 0.0))
        head_w = totals(jnp.where(here[None], images[...], 0.0))
        ahead = panel[following] - jnp.sum(vecs[...] * head_w + images[...] * head_v, axis=0)
        vecs[step] = vector
        lead_v = total(jnp.where(here, vector, 0.0))
        half_tau = 0.5 * tau * tau
        arrived(parts_in.at[step, pl.ds(0, 2 * rows - 1)], parts_sem.at[step])
        for r in range(rows):
            whole[r * halves : (r + 1) * halves, :] = parts_in[step, r] + parts_in[step, rows + r]
        change = whole[...] - known
        along = half_tau * total(change * vector)
        lead_w = tau * total(jnp.where(here, change, 0.0)) - along * lead_v
        image = tau * change - along * vector
        images[step] = image
        column = ahead - vector * lead_w - image * lead_v
        return column, diagonal, offdiag

    nothing = jnp.zeros((8, tile), jnp.float32)
    _, diagonal, offdiag = lax.fori_loop(0, PB, advance, (panel[0], nothing, nothing))
    diag_ref[...] = diagonal[0:1, 0:PB]
    off_ref[...] = offdiag[0:1, 0:PB]
    left_v = [vecs[:, pl.ds(halves * row + h, 1), :].reshape(PB, tile) for h in range(halves)]
    left_w = [images[:, pl.ds(halves * row + h, 1), :].reshape(PB, tile) for h in range(halves)]
    for b in range(blocks):
        t = b * cols + col
        e = (t % rows) * halves + t // rows
        right_v = vecs[:, pl.ds(e, 1), :].reshape(PB, tile)
        right_w = images[:, pl.ds(e, 1), :].reshape(PB, tile)
        for h in range(halves):
            change = lax.dot_general(
                jnp.concatenate([left_v[h], left_w[h]], axis=0),
                jnp.concatenate([right_w, right_v], axis=0),
                (((0,), (0,)), ((), ())),
                precision=lax.Precision.HIGHEST,
                preferred_element_type=jnp.float32,
            )
            block = a_ref[h * tile : (h + 1) * tile, b * tile : (b + 1) * tile]
            updated_ref[pl.ds(h * tile * blocks + b, tile, stride=blocks), :] = block - change


    def sent(ref):
        pltpu.make_async_copy(ref, ref, send_sem).wait()

    @pl.when(col == 0)
    def _():
        sent(panel_in.at[pl.ds(0, len(around))])

    @pl.when(pair == 0)
    def _():
        sent(panel_in.at[pl.ds(0, rows)])
        sent(panel_in.at[pl.ds(0, rows - 1)])

    for _ in range(3):
        sent(a_ref)
    sent(eig_cols.at[pl.ds(0, 7)])
    sent(eig_cols.at[pl.ds(0, rows // 2)])
    sent(psi_rows.at[pl.ds(0, 7)])

    def drain(step, carry):
        sent(parts_in.at[step, pl.ds(0, 2 * rows - 1)])
        return carry

    lax.fori_loop(0, PB, drain, 0)

    for n in range(2):
        sent(by_row.at[n, 0, pl.ds(0, rows - 1)])
        sent(by_col.at[n, 0, pl.ds(0, cols - 1)])
        sent(by_row.at[n, pl.ds(0, 7)])
        sent(by_col.at[n, pl.ds(0, 7)])
        sent(by_col.at[n, pl.ds(0, rows // 2)])


def reduce_and_rotate(psi, hpsi, eigvec, rows, cols):
    height, width = eigvec.shape
    tile = 128
    halves = height // tile
    tiles = rows * halves
    depth = cols * psi.shape[0]
    vmem = pl.BlockSpec(memory_space=pltpu.VMEM)
    block = pltpu.VMEM((height, width), jnp.float32)
    vectors = pltpu.VMEM((PB, tiles, tile), jnp.float32)
    laid = jax.ShapeDtypeStruct((height * width // tile, tile), jnp.float32)
    return pl.pallas_call(
        whole_kernel,
        out_shape=(
            laid,
            laid,
            jax.ShapeDtypeStruct((1, PB), jnp.float32),
            jax.ShapeDtypeStruct((1, PB), jnp.float32),
            jax.ShapeDtypeStruct((depth * width // tile, tile), psi.dtype),
        ),
        in_specs=[vmem] * 3,
        out_specs=(vmem,) * 5,
        scratch_shapes=[
            pltpu.VMEM((2, cols, rows, psi.shape[0], height), psi.dtype),
            pltpu.VMEM((2, rows, cols, psi.shape[0], width), psi.dtype),
            block,
            block,
            pltpu.VMEM((cols, *psi.shape), psi.dtype),
            pltpu.VMEM((rows, *eigvec.shape), eigvec.dtype),
            pltpu.VMEM((depth, width), jnp.float32),
            pltpu.VMEM((depth * width // tile, tile), jnp.float32),
            pltpu.VMEM((cols // 2, height, width), jnp.float32),
            pltpu.VMEM((rows, PB, halves, tile), jnp.float32),
            vectors,
            vectors,
            vectors,
            pltpu.VMEM((tiles, tile), jnp.float32),
            pltpu.VMEM((height, tile), jnp.float32),
            pltpu.VMEM((PB, halves, tile), jnp.float32),
            pltpu.VMEM((PB, 2 * rows, halves, tile), jnp.float32),
            pltpu.VMEM((tiles, tile), jnp.float32),
            pltpu.SemaphoreType.DMA,
            pltpu.SemaphoreType.DMA((2, 2)),
            pltpu.SemaphoreType.DMA((2, 2, 9)),
            pltpu.SemaphoreType.DMA((2,)),
            pltpu.SemaphoreType.DMA((6,)),
            pltpu.SemaphoreType.DMA((2,)),
            pltpu.SemaphoreType.DMA((PB,)),
            pltpu.SemaphoreType.DMA((9,)),
            pltpu.SemaphoreType.DMA,
            pltpu.SemaphoreType.DMA((9,)),
        ],
        compiler_params=pltpu.CompilerParams(
            collective_id=0, has_side_effects=True, vmem_limit_bytes=56 * 1024 * 1024
        ),
        name="whole",
    )(psi, hpsi, eigvec)


def on_device(psi, hpsi, eigvec):
    row_tiles, _, tile_size, col_tiles = eigvec.shape[:4]
    correlation, updated, diagonal, offdiag, rotated = reduce_and_rotate(
        psi,
        hpsi,
        eigvec.reshape(row_tiles * tile_size, col_tiles * tile_size),
        lax.axis_size("row"),
        lax.axis_size("col"),
    )
    tile_shape = (row_tiles, 1, tile_size, col_tiles, 1, tile_size)
    return (
        correlation.reshape(tile_shape),
        updated.reshape(tile_shape),
        diagonal.reshape(PB),
        offdiag.reshape(PB),
        rotated.reshape(-1, col_tiles, 1, tile_size),
    )


def solution(mesh):
    return jax.shard_map(
        on_device,
        mesh=mesh,
        in_specs=(
            P(("row", "col"), None),
            P(("row", "col"), None),
            P(None, "row", None, None, "col", None),
        ),
        out_specs=(
            P(None, "row", None, None, "col", None),
            P(None, "row", None, None, "col", None),
            P(),
            P(),
            P("row", None, "col", None),
        ),
        check_vma=False,
    )
```

```python
import jax
import jax.numpy as jnp
from jax import lax
from jax.experimental import pallas as pl
from jax.experimental.pallas import tpu as pltpu
from jax.sharding import PartitionSpec as P

PB = 16
MESH = pl.DeviceIdType.MESH


def split_three(x):
    high = x.astype(jnp.bfloat16)
    rest = x - high.astype(jnp.float32)
    mid = rest.astype(jnp.bfloat16)
    low = (rest - mid.astype(jnp.float32)).astype(jnp.bfloat16)
    return high, mid, low


def lattice(row, col):
    pair = {"row": lax.div(row, 8), "col": lax.div(col, 4)}
    ring = {"row": lax.rem(lax.div(row, 2), 4), "col": lax.rem(col, 4)}
    return pair, ring


def whole_kernel(
    psi_ref,
    hpsi_ref,
    eig_ref,
    corr_ref,
    updated_ref,
    diag_ref,
    off_ref,
    rotated_ref,
    by_row,
    by_col,
    total_s,
    a_ref,
    psi_rows,
    eig_cols,
    rotated,
    rotated_tiles,
    a_plane,
    panel_in,
    panel,
    vecs,
    images,
    vec,
    lanes_sum,
    parts_out,
    parts_in,
    whole,
    ends,
    send_sem,
    swap_sem,
    gather_sem,
    gather_core,
    ring_sem,
    panel_sem,
    parts_sem,
    eig_sem,
    core_sem,
    psi_sem,
    back_sem,
):
    rows = lax.axis_size("row")
    cols = lax.axis_size("col")
    row = lax.axis_index("row")
    col = lax.axis_index("col")
    tile = 128
    height, width = a_ref.shape
    halves, blocks = height // tile, width // tile
    tiles = rows * halves
    turns = cols // 2
    pairs, rings = lattice(row, col)
    pair, ring = pairs["col"], rings["col"]
    inputs = (psi_ref, hpsi_ref)
    core = lax.rem(row, 2)

    def place(axis, across, along):
        p = lax.rem(pairs[axis] + across, 2)
        q = lax.rem(rings[axis] + along + 4, 4)
        return p * 8 + q * 2 + core if axis == "row" else p * 4 + q

    order = sorted(
        ((d, e) for d in range(rows) for e in range(2) if d + e > 0),
        key=lambda de: -min(de[0], rows - de[0]) - 4 * de[1],
    )
    peers = [
        {"row": lax.rem(row + d, rows), "col": lax.rem(pair + e, 2) * turns + ring}
        for d, e in order
    ]
    around = [{"row": row, "col": pair * turns + lax.rem(ring + d, turns)} for d in (1, 3, 2)]
    beyond = [
        {"row": row, "col": (1 - pair) * turns + lax.rem(ring + d, turns)} for d in (1, 3, 2)
    ]
    row_order = sorted(range(1, rows), key=lambda d: -min(d, rows - d))
    row_peers = [lax.rem(row + d, rows) for d in row_order]
    col_peers = [lax.rem(col + d, cols) for d in range(1, cols)]
    chip = lax.div(row, 2)
    head = row - core + 1
    hops = {(0, 0): 0, (1, 0): 1, (0, 1): 2, (1, 1): 1}
    steps = [(x, z, e) for x in range(2) for z in range(4) for e in range(2) if x + z + e > 0]
    heads = [
        {
            "row": lax.rem(pairs["row"] + x, 2) * 8 + lax.rem(rings["row"] + z, 4) * 2 + 1,
            "col": lax.rem(pair + e, 2) * turns + ring,
        }
        for x, z, e in sorted(steps, key=lambda q: -hops[q[0], q[2]] - min(q[1], 4 - q[1]))
    ]
    aside = [{**peer, "row": row + 1 - 2 * core} for peer in around]
    greeted = peers + around + beyond + aside
    barrier = pltpu.get_barrier_semaphore()
    for peer in greeted:
        pl.semaphore_signal(barrier, inc=1, device_id=peer, device_id_type=MESH)
    pl.semaphore_wait(barrier, len(greeted))

    def send(source, target, sem, where):
        pltpu.make_async_remote_copy(
            src_ref=source,
            dst_ref=target,
            send_sem=send_sem,
            recv_sem=sem,
            device_id={"row": row, "col": col, **where},
            device_id_type=MESH,
        ).start()

    def lanes(tile_index):
        return pl.ds(pl.multiple_of(tile_index * tile, tile), tile)

    def arrived(ref, sem):
        pltpu.make_async_copy(ref, ref, sem).wait()

    for n, source in enumerate(inputs):
        for r in row_peers:
            for h in range(halves):
                send(
                    source.at[:, lanes(h * rows + r)],
                    by_row.at[n, col, row, :, h * tile : (h + 1) * tile],
                    swap_sem.at[n, 0],
                    {"row": r},
                )
        for c in col_peers:
            for b in range(blocks):
                send(
                    source.at[:, lanes(b * cols + c)],
                    by_col.at[n, row, col, :, b * tile : (b + 1) * tile],
                    swap_sem.at[n, 1],
                    {"col": c},
                )
    for n, source in enumerate(inputs):
        for h in range(halves):
            by_row[n, col, row, :, h * tile : (h + 1) * tile] = source[:, lanes(h * rows + row)]
        for b in range(blocks):
            by_col[n, row, col, :, b * tile : (b + 1) * tile] = source[:, lanes(b * cols + col)]

    kinds = [(n, part) for n in range(2) for part in range(2)]
    axes = ("col", "row")
    held = (by_row, by_col)

    def gathered(n, part, across, along, half=None):
        whole = held[part].at[n, place(axes[part], across, along)]
        if half is None:
            return whole
        size = whole.shape[0] // 2
        return whole.at[pl.ds(half * size, size)]

    def along_ring(n, part, across, along, way, half, sem):
        what = gathered(n, part, across, along, half)
        where = {axes[part]: place(axes[part], 0, way)}
        send(what, what, gather_sem.at[n, part, sem], where)

    def to_core(n, part, across, along, half=None):
        if part == 1:
            what = gathered(n, part, across, along, half)
            send(what, what, gather_core.at[n], {"row": row + 1 - 2 * core})

    def wait_ring(n, part, across, along, half, sem):
        arrived(gathered(n, part, across, along, half), gather_sem.at[n, part, sem])

    for n, part in kinds:
        count = (rows if part == 0 else cols) - 1
        mine = (col if part == 0 else row,)
        arrived(held[part].at[n, mine[0], pl.ds(0, count)], swap_sem.at[n, part])
        along_ring(n, part, 0, 0, 1, None, 0)
        along_ring(n, part, 0, 0, -1, None, 1)
        what = gathered(n, part, 0, 0)
        send(what, what, gather_sem.at[n, part, 2], {axes[part]: place(axes[part], 1, 0)})
        to_core(n, part, 0, 0)
    for n, part in kinds:
        wait_ring(n, part, 0, -1, None, 0)
        along_ring(n, part, 0, -1, 1, 0, 3)
        to_core(n, part, 0, -1)
        wait_ring(n, part, 0, 1, None, 1)
        along_ring(n, part, 0, 1, -1, 1, 4)
        to_core(n, part, 0, 1)
        wait_ring(n, part, 1, 0, None, 2)
        along_ring(n, part, 1, 0, 1, None, 5)
        along_ring(n, part, 1, 0, -1, None, 6)
        to_core(n, part, 1, 0)
    for n, part in kinds:
        wait_ring(n, part, 0, 2, 0, 3)
        to_core(n, part, 0, 2, 0)
        wait_ring(n, part, 0, 2, 1, 4)
        to_core(n, part, 0, 2, 1)
        wait_ring(n, part, 1, -1, None, 5)
        along_ring(n, part, 1, -1, 1, 0, 7)
        to_core(n, part, 1, -1)
        wait_ring(n, part, 1, 1, None, 6)
        along_ring(n, part, 1, 1, -1, 1, 8)
        to_core(n, part, 1, 1)
    for n, part in kinds:
        wait_ring(n, part, 1, 2, 0, 7)
        to_core(n, part, 1, 2, 0)
        wait_ring(n, part, 1, 2, 1, 8)
        to_core(n, part, 1, 2, 1)
    for n in range(2):
        arrived(by_col.at[n, pl.ds(0, rows // 2)], gather_core.at[n])


    def eig_place(across, along):
        return place("row", across, along)

    def psi_place(across, along):
        return place("col", across, along)

    def piece(held, index, half):
        whole = held.at[index]
        if half is None:
            return whole
        size = whole.shape[0] // 2
        return whole.at[pl.ds(half * size, size)]

    def eig_send(across, along, way, half, sem):
        what = piece(eig_cols, eig_place(across, along), half)
        to = eig_place(1, 0) if way is None else eig_place(0, way)
        send(what, what, eig_sem.at[sem], {"row": to, "col": col})

    def eig_core(across, along, half):
        what = piece(eig_cols, eig_place(across, along), half)
        send(what, what, core_sem, {"row": row + 1 - 2 * core, "col": col})

    def eig_wait(across, along, half, sem):
        arrived(piece(eig_cols, eig_place(across, along), half), eig_sem.at[sem])

    def psi_send(across, along, way, half, sem):
        what = piece(psi_rows, psi_place(across, along), half)
        to = psi_place(1, 0) if way is None else psi_place(0, way)
        send(what, what, psi_sem.at[sem], {"row": row, "col": to})

    def psi_wait(across, along, half, sem):
        arrived(piece(psi_rows, psi_place(across, along), half), psi_sem.at[sem])

    depth = rows * by_row.shape[3]

    def row_block(n, c):
        return by_row[n, c].reshape(depth, halves * tile)

    def col_block(n, c):
        return by_col[n, :, c].reshape(depth, blocks * tile)

    def product(left, right):
        return lax.dot_general(
            left, right, (((0,), (0,)), ((), ())), preferred_element_type=jnp.float32
        )

    def add_s(c, carry):
        total_s[...] += product(row_block(0, c), col_block(0, c))
        return carry

    def add_a(c, carry):
        a_ref[...] += product(row_block(0, c), col_block(1, c)) + product(
            row_block(1, c), col_block(0, c)
        )
        return carry

    a_ref[...] = jnp.zeros_like(a_ref)
    lax.fori_loop(0, cols, add_a, 0)
    a_ref[...] = 0.5 * a_ref[...]

    def to_heads(source, target, recv):
        for peer in heads:
            send(source, target, recv, peer)

    @pl.when(col == 0)
    def _():
        for half in range(halves):
            first = a_ref[half * tile : (half + 1) * tile, 0:tile]
            panel_in[row, :, half, :] = jnp.transpose(first)[0:PB, :]
        mine = panel_in.at[row]
        for peer in around:
            send(mine, mine, panel_sem.at[core], {**peer, "row": head})

        @pl.when(core == 0)
        def _():
            send(mine, mine, panel_sem.at[0], {"row": head})

    above, below = lax.rem(ring + 1, turns), lax.rem(ring + turns - 1, turns)
    half_rows = height // 2

    def part_of(where, k, half):
        first = pl.multiple_of(k * height + half * half_rows, half_rows)
        return a_plane.at[where, pl.ds(first, half_rows)]

    for half in range(2):
        for way, part in ((0, half), (1, 1 - half)):
            send(
                a_ref.at[pl.ds(part * half_rows, half_rows)],
                part_of(ring, core, part),
                ring_sem.at[core, 2 * way + part],
                {**around[way], "row": head},
            )

    own_rows = pl.ds(pl.multiple_of(core * height, height), height)

    @pl.when(core == 0)
    def _():
        send(a_ref, a_plane.at[ring, own_rows], back_sem.at[3], {"row": head})

    @pl.when((core == 1) & (pair == 0))
    def _():
        arrived(panel_in.at[row - core], panel_sem.at[0])

        @pl.when(ring > 0)
        def _():
            arrived(panel_in.at[row], panel_sem.at[1])

        both = panel_in.at[pl.ds(row - core, 2)]
        to_heads(both, both, panel_sem.at[2])

    eig_cols[row] = eig_ref[...]
    psi_rows[col] = psi_ref[...]
    eig_send(0, 0, 1, None, 0)
    eig_send(0, 0, -1, None, 1)
    eig_send(0, 0, None, None, 2)
    eig_core(0, 0, None)
    psi_send(0, 0, None, None, 2)


    spot = lax.broadcasted_iota(jnp.int32, (tiles, tile), 0)
    lane = lax.broadcasted_iota(jnp.int32, (tiles, tile), 1)
    positions = ((spot % halves) * rows + spot // halves) * tile + lane
    slot = lax.broadcasted_iota(jnp.int32, (8, tile), 1)

    @pl.when(core == 1)
    def _():
        a_plane[ring, height : 2 * height, :] = a_ref[...]
        vecs[...] = jnp.zeros_like(vecs)
        images[...] = jnp.zeros_like(images)

        @pl.when(pair == 0)
        def _():
            arrived(panel_in.at[pl.ds(0, rows - 2)], panel_sem.at[2])

        @pl.when(pair > 0)
        def _():
            arrived(panel_in, panel_sem.at[2])

        for r in range(rows):
            panel[:, r * halves : (r + 1) * halves, :] = panel_in[r]
        for k in range(2):
            arrived(part_of(below, k, 0), ring_sem.at[k, 0])
            send(part_of(below, k, 0), part_of(below, k, 0), ring_sem.at[k, 4], around[0])
            arrived(part_of(above, k, 1), ring_sem.at[k, 3])
            send(part_of(above, k, 1), part_of(above, k, 1), ring_sem.at[k, 5], around[1])

    eig_wait(0, -1, None, 0)
    eig_send(0, -1, 1, 0, 3)
    eig_core(0, -1, None)
    eig_wait(0, 1, None, 1)
    eig_send(0, 1, -1, 1, 4)
    eig_core(0, 1, None)
    eig_wait(1, 0, None, 2)
    eig_send(1, 0, 1, None, 5)
    eig_send(1, 0, -1, None, 6)
    eig_core(1, 0, None)
    psi_send(0, 0, 1, None, 0)
    psi_send(0, 0, -1, None, 1)
    psi_wait(1, 0, None, 2)
    psi_send(1, 0, 1, None, 5)
    psi_send(1, 0, -1, None, 6)
    across = lax.rem(ring + 2, turns)

    def background(step):
        @pl.when(step == 0)
        def _():
            eig_wait(0, 2, 0, 3)
            eig_core(0, 2, 0)
            eig_wait(0, 2, 1, 4)
            eig_core(0, 2, 1)
            eig_wait(1, -1, None, 5)
            eig_send(1, -1, 1, 0, 7)
            eig_core(1, -1, None)
            eig_wait(1, 1, None, 6)
            eig_send(1, 1, -1, 1, 8)
            eig_core(1, 1, None)

        @pl.when(step == 2)
        def _():
            eig_wait(1, 2, 0, 7)
            eig_core(1, 2, 0)
            eig_wait(1, 2, 1, 8)
            eig_core(1, 2, 1)
            psi_wait(0, -1, None, 0)
            psi_send(0, -1, 1, 0, 3)
            psi_wait(0, 1, None, 1)
            psi_send(0, 1, -1, 1, 4)

        @pl.when(step == 3)
        def _():
            total_s[...] = jnp.zeros_like(total_s)
            lax.fori_loop(0, cols, add_s, 0)

        @pl.when(step == 5)
        def _():
            scale = 1.0 / (rows * cols * psi_ref.shape[0])
            for b in range(blocks):
                corr_ref[pl.ds(b, height, stride=blocks), :] = scale * total_s[
                    :, b * tile : (b + 1) * tile
                ]

        @pl.when(step == 4)
        def _():
            psi_wait(1, -1, None, 5)
            psi_send(1, -1, 1, 0, 7)
            psi_wait(1, 1, None, 6)
            psi_send(1, 1, -1, 1, 8)

        @pl.when(step == 6)
        def _():
            for half in range(2):
                psi_wait(0, 2, half, 3 + half)
                psi_wait(1, 2, half, 7 + half)
            arrived(eig_cols.at[pl.ds(0, rows // 2)], core_sem)
            rotated[...] = jnp.zeros_like(rotated)

        @pl.when((step >= PB // 2 - 1) & (step < PB - 1))
        def _():
            per = rows // (PB // 2)
            for k in range(per):
                r = (step - PB // 2 + 1) * per + k
                left = [
                    psi_rows[:, :, pl.ds(pl.multiple_of((h * rows + r) * tile, tile), tile)]
                    for h in range(halves)
                ]
                left = jnp.concatenate([x.reshape(-1, tile) for x in left], axis=1)
                rotated[...] += jnp.dot(left, eig_cols[r], preferred_element_type=jnp.float32)

        @pl.when(step == PB - 1)
        def _():
            depth = rotated.shape[0]
            for b in range(blocks):
                rotated_tiles[pl.ds(b, depth, stride=blocks), :] = rotated[
                    :, b * tile : (b + 1) * tile
                ]
            rotated_ref[...] = rotated_tiles[...].astype(rotated_ref.dtype)

    def total(x):
        return jnp.sum(x, axis=(0, 1), keepdims=True)

    def totals(x):
        return jnp.sum(x, axis=(1, 2), keepdims=True)

    def reflector(column, step):
        at = total(jnp.where(positions == step, column, 0.0))
        pivot = total(jnp.where(positions == step + 1, column, 0.0))
        under = positions > step + 1
        tail = total(jnp.where(under, column * column, 0.0))
        length = jnp.sqrt(pivot * pivot + tail)
        beta = jnp.where(pivot >= 0.0, -length, length)
        tau = (beta - pivot) / beta
        scale = 1.0 / (pivot - beta)
        vector = jnp.where(positions == step + 1, 1.0, jnp.where(under, column * scale, 0.0))
        return at, beta, tau, vector

    def advance(step, carry):
        column, diagonal, offdiag = carry
        at, beta, tau, vector = reflector(column, step)
        diagonal = jnp.where(slot == step, at, diagonal)
        offdiag = jnp.where(slot == step, beta, offdiag)
        vec[...] = vector
        spread = []
        for y in range(turns):
            for b in range(blocks):
                t = b * cols + pair * turns + y
                e = lax.rem(t, rows) * halves + lax.div(t, rows)
                spread.append(jnp.broadcast_to(vec[pl.ds(e, 1), :], (8, tile)))

        def band(group, _):
            at_rows = pl.ds(pl.multiple_of(group * 8, 8), 8)
            sums = [jnp.zeros((8, tile), jnp.float32) for _ in range(4)]
            for y in range(turns):
                for b in range(blocks):
                    block = a_plane[y, at_rows, b * tile : (b + 1) * tile]
                    sums[b] = sums[b] + block * spread[y * blocks + b]
            lanes_sum[at_rows, :] = (sums[0] + sums[1]) + (sums[2] + sums[3])
            return 0

        lax.fori_loop(0, 2 * height // 8, band, 0, unroll=4)
        ones = jnp.ones((16, tile), jnp.bfloat16)
        product = jnp.zeros((16, 2 * height), jnp.float32)
        for piece in split_three(lanes_sum[...]):
            product = product + lax.dot_general(
                ones, piece, (((1,), (1,)), ((), ())), preferred_element_type=jnp.float32
            )
        for q in range(2 * halves):
            parts_out[step, q : q + 1, :] = product[0:1, q * tile : (q + 1) * tile]
        mine = pair * (rows // 2) + chip
        to_heads(parts_out.at[step], parts_in.at[step, mine], parts_sem.at[step])
        parts_in[step, mine] = parts_out[step]
        background(step)
        by_vecs = totals(vecs[...] * vector[None])
        by_images = totals(images[...] * vector[None])
        known = jnp.sum(vecs[...] * by_images + images[...] * by_vecs, axis=0)
        following = jnp.minimum(step + 1, PB - 1)
        here = positions == following
        head_v = totals(jnp.where(here[None], vecs[...], 0.0))
        head_w = totals(jnp.where(here[None], images[...], 0.0))
        ahead = panel[following] - jnp.sum(vecs[...] * head_w + images[...] * head_v, axis=0)
        vecs[step] = vector
        send(vecs.at[step], vecs.at[step], back_sem.at[0], {"row": row - core})
        lead_v = total(jnp.where(here, vector, 0.0))
        half_tau = 0.5 * tau * tau
        arrived(parts_in.at[step, pl.ds(0, rows - 1)], parts_sem.at[step])
        for m in range(rows // 2):
            whole[m * 2 * halves : (m + 1) * 2 * halves, :] = (
                parts_in[step, m] + parts_in[step, rows // 2 + m]
            )
        change = whole[...] - known
        along = half_tau * total(change * vector)
        lead_w = tau * total(jnp.where(here, change, 0.0)) - along * lead_v
        image = tau * change - along * vector
        images[step] = image
        send(images.at[step], images.at[step], back_sem.at[1], {"row": row - core})
        column = ahead - vector * lead_w - image * lead_v
        return column, diagonal, offdiag

    @pl.when(core == 1)
    def _():
        for k in range(2):
            arrived(part_of(below, k, 1), ring_sem.at[k, 1])
            arrived(part_of(above, k, 0), ring_sem.at[k, 2])
            arrived(part_of(across, k, 0), ring_sem.at[k, 4])
            arrived(part_of(across, k, 1), ring_sem.at[k, 5])
        arrived(a_plane.at[ring, pl.ds(0, height)], back_sem.at[3])
        nothing = jnp.zeros((8, tile), jnp.float32)
        _, diagonal, offdiag = lax.fori_loop(0, PB, advance, (panel[0], nothing, nothing))
        ends[0] = diagonal
        ends[1] = offdiag
        send(ends, ends, back_sem.at[2], {"row": row - core})

    @pl.when(core == 0)
    def _():
        def wait_step(step, carry):
            background(step)
            return carry

        lax.fori_loop(0, PB, wait_step, 0)
        arrived(vecs, back_sem.at[0])
        arrived(images, back_sem.at[1])
        arrived(ends, back_sem.at[2])

    diag_ref[...] = ends[0, 0:1, 0:PB]
    off_ref[...] = ends[1, 0:1, 0:PB]
    left_v = [vecs[:, pl.ds(halves * row + h, 1), :].reshape(PB, tile) for h in range(halves)]
    left_w = [images[:, pl.ds(halves * row + h, 1), :].reshape(PB, tile) for h in range(halves)]
    for b in range(blocks):
        t = b * cols + col
        e = (t % rows) * halves + t // rows
        right_v = vecs[:, pl.ds(e, 1), :].reshape(PB, tile)
        right_w = images[:, pl.ds(e, 1), :].reshape(PB, tile)
        for h in range(halves):
            change = lax.dot_general(
                jnp.concatenate([left_v[h], left_w[h]], axis=0),
                jnp.concatenate([right_w, right_v], axis=0),
                (((0,), (0,)), ((), ())),
                precision=lax.Precision.HIGHEST,
                preferred_element_type=jnp.float32,
            )
            block = a_ref[h * tile : (h + 1) * tile, b * tile : (b + 1) * tile]
            updated_ref[pl.ds(h * tile * blocks + b, tile, stride=blocks), :] = block - change


    def sent(ref):
        pltpu.make_async_copy(ref, ref, send_sem).wait()

    @pl.when(col == 0)
    def _():
        sent(panel_in.at[pl.ds(0, len(around))])

    for _ in range(2):
        sent(a_ref)

    @pl.when(core == 0)
    def _():
        sent(a_ref)

        @pl.when(col == 0)
        def _():
            sent(panel_in.at[0])

    @pl.when(core == 1)
    def _():
        @pl.when(pair == 0)
        def _():
            sent(panel_in)
            sent(panel_in.at[pl.ds(0, rows - 2)])

        for _ in range(2):
            sent(a_ref)
        sent(vecs)
        sent(images)
        sent(ends)

    sent(eig_cols.at[pl.ds(0, 7)])
    sent(eig_cols.at[pl.ds(0, rows // 2)])
    sent(psi_rows.at[pl.ds(0, 7)])

    def drain(step, carry):
        sent(parts_in.at[step, pl.ds(0, rows - 1)])
        return carry

    @pl.when(core == 1)
    def _():
        lax.fori_loop(0, PB, drain, 0)

    for n in range(2):
        sent(by_row.at[n, 0, pl.ds(0, rows - 1)])
        sent(by_col.at[n, 0, pl.ds(0, cols - 1)])
        sent(by_row.at[n, pl.ds(0, 7)])
        sent(by_col.at[n, pl.ds(0, 7)])
        sent(by_col.at[n, pl.ds(0, rows // 2)])


def reduce_and_rotate(psi, hpsi, eigvec, rows, cols):
    height, width = eigvec.shape
    tile = 128
    halves = height // tile
    tiles = rows * halves
    depth = cols * psi.shape[0]
    vmem = pl.BlockSpec(memory_space=pltpu.VMEM)
    block = pltpu.VMEM((height, width), jnp.float32)
    vectors = pltpu.VMEM((PB, tiles, tile), jnp.float32)
    laid = jax.ShapeDtypeStruct((height * width // tile, tile), jnp.float32)
    return pl.pallas_call(
        whole_kernel,
        out_shape=(
            laid,
            laid,
            jax.ShapeDtypeStruct((1, PB), jnp.float32),
            jax.ShapeDtypeStruct((1, PB), jnp.float32),
            jax.ShapeDtypeStruct((depth * width // tile, tile), psi.dtype),
        ),
        in_specs=[vmem] * 3,
        out_specs=(vmem,) * 5,
        scratch_shapes=[
            pltpu.VMEM((2, cols, rows, psi.shape[0], height), psi.dtype),
            pltpu.VMEM((2, rows, cols, psi.shape[0], width), psi.dtype),
            block,
            block,
            pltpu.VMEM((cols, *psi.shape), psi.dtype),
            pltpu.VMEM((rows, *eigvec.shape), eigvec.dtype),
            pltpu.VMEM((depth, width), jnp.float32),
            pltpu.VMEM((depth * width // tile, tile), jnp.float32),
            pltpu.VMEM((cols // 2, 2 * height, width), jnp.float32),
            pltpu.VMEM((rows, PB, halves, tile), jnp.float32),
            vectors,
            vectors,
            vectors,
            pltpu.VMEM((tiles, tile), jnp.float32),
            pltpu.VMEM((2 * height, tile), jnp.float32),
            pltpu.VMEM((PB, 2 * halves, tile), jnp.float32),
            pltpu.VMEM((PB, rows, 2 * halves, tile), jnp.float32),
            pltpu.VMEM((tiles, tile), jnp.float32),
            pltpu.VMEM((2, 8, tile), jnp.float32),
            pltpu.SemaphoreType.DMA,
            pltpu.SemaphoreType.DMA((2, 2)),
            pltpu.SemaphoreType.DMA((2, 2, 9)),
            pltpu.SemaphoreType.DMA((2,)),
            pltpu.SemaphoreType.DMA((2, 6)),
            pltpu.SemaphoreType.DMA((3,)),
            pltpu.SemaphoreType.DMA((PB,)),
            pltpu.SemaphoreType.DMA((9,)),
            pltpu.SemaphoreType.DMA,
            pltpu.SemaphoreType.DMA((9,)),
            pltpu.SemaphoreType.DMA((4,)),
        ],
        compiler_params=pltpu.CompilerParams(
            collective_id=0, has_side_effects=True, vmem_limit_bytes=56 * 1024 * 1024
        ),
        name="whole",
    )(psi, hpsi, eigvec)


def on_device(psi, hpsi, eigvec):
    row_tiles, _, tile_size, col_tiles = eigvec.shape[:4]
    correlation, updated, diagonal, offdiag, rotated = reduce_and_rotate(
        psi,
        hpsi,
        eigvec.reshape(row_tiles * tile_size, col_tiles * tile_size),
        lax.axis_size("row"),
        lax.axis_size("col"),
    )
    tile_shape = (row_tiles, 1, tile_size, col_tiles, 1, tile_size)
    return (
        correlation.reshape(tile_shape),
        updated.reshape(tile_shape),
        diagonal.reshape(PB),
        offdiag.reshape(PB),
        rotated.reshape(-1, col_tiles, 1, tile_size),
    )


def solution(mesh):
    return jax.shard_map(
        on_device,
        mesh=mesh,
        in_specs=(
            P(("row", "col"), None),
            P(("row", "col"), None),
            P(None, "row", None, None, "col", None),
        ),
        out_specs=(
            P(None, "row", None, None, "col", None),
            P(None, "row", None, None, "col", None),
            P(),
            P(),
            P("row", None, "col", None),
        ),
        check_vma=False,
    )
```

```python
import jax
import jax.numpy as jnp
from jax import lax
from jax.experimental import pallas as pl
from jax.experimental.pallas import tpu as pltpu
from jax.sharding import PartitionSpec as P

PB = 16
MESH = pl.DeviceIdType.MESH


def split_three(x):
    high = x.astype(jnp.bfloat16)
    rest = x - high.astype(jnp.float32)
    mid = rest.astype(jnp.bfloat16)
    low = (rest - mid.astype(jnp.float32)).astype(jnp.bfloat16)
    return high, mid, low


def lattice(row, col):
    pair = {"row": lax.div(row, 8), "col": lax.div(col, 4)}
    ring = {"row": lax.rem(lax.div(row, 2), 4), "col": lax.rem(col, 4)}
    return pair, ring


def whole_kernel(
    psi_ref,
    hpsi_ref,
    eig_ref,
    corr_ref,
    updated_ref,
    diag_ref,
    off_ref,
    rotated_ref,
    by_row,
    by_col,
    total_s,
    a_ref,
    psi_rows,
    eig_cols,
    rotated,
    rotated_tiles,
    a_plane,
    panel_in,
    panel,
    vecs,
    images,
    vec,
    lanes_sum,
    parts_out,
    parts_in,
    whole,
    ends,
    send_sem,
    swap_sem,
    gather_sem,
    gather_core,
    ring_sem,
    panel_sem,
    parts_sem,
    eig_sem,
    core_sem,
    psi_sem,
    back_sem,
):
    rows = lax.axis_size("row")
    cols = lax.axis_size("col")
    row = lax.axis_index("row")
    col = lax.axis_index("col")
    tile = 128
    height, width = a_ref.shape
    halves, blocks = height // tile, width // tile
    tiles = rows * halves
    turns = cols // 2
    pairs, rings = lattice(row, col)
    pair, ring = pairs["col"], rings["col"]
    inputs = (psi_ref, hpsi_ref)
    core = lax.rem(row, 2)

    def place(axis, across, along):
        p = lax.rem(pairs[axis] + across, 2)
        q = lax.rem(rings[axis] + along + 4, 4)
        return p * 8 + q * 2 + core if axis == "row" else p * 4 + q

    order = sorted(
        ((d, e) for d in range(rows) for e in range(2) if d + e > 0),
        key=lambda de: -min(de[0], rows - de[0]) - 4 * de[1],
    )
    peers = [
        {"row": lax.rem(row + d, rows), "col": lax.rem(pair + e, 2) * turns + ring}
        for d, e in order
    ]
    around = [{"row": row, "col": pair * turns + lax.rem(ring + d, turns)} for d in (1, 3, 2)]
    beyond = [
        {"row": row, "col": (1 - pair) * turns + lax.rem(ring + d, turns)} for d in (1, 3, 2)
    ]
    row_order = sorted(range(1, rows), key=lambda d: -min(d, rows - d))
    row_peers = [lax.rem(row + d, rows) for d in row_order]
    col_peers = [lax.rem(col + d, cols) for d in range(1, cols)]
    chip = lax.div(row, 2)
    head = row - core + 1
    hops = {(0, 0): 0, (1, 0): 1, (0, 1): 2, (1, 1): 1}
    steps = [(x, z, e) for x in range(2) for z in range(4) for e in range(2) if x + z + e > 0]
    heads = [
        {
            "row": lax.rem(pairs["row"] + x, 2) * 8 + lax.rem(rings["row"] + z, 4) * 2 + 1,
            "col": lax.rem(pair + e, 2) * turns + ring,
        }
        for x, z, e in sorted(steps, key=lambda q: -hops[q[0], q[2]] - min(q[1], 4 - q[1]))
    ]
    aside = [{**peer, "row": row + 1 - 2 * core} for peer in around]
    greeted = peers + around + beyond + aside
    barrier = pltpu.get_barrier_semaphore()
    for peer in greeted:
        pl.semaphore_signal(barrier, inc=1, device_id=peer, device_id_type=MESH)
    pl.semaphore_wait(barrier, len(greeted))

    def send(source, target, sem, where):
        pltpu.make_async_remote_copy(
            src_ref=source,
            dst_ref=target,
            send_sem=send_sem,
            recv_sem=sem,
            device_id={"row": row, "col": col, **where},
            device_id_type=MESH,
        ).start()

    def lanes(tile_index):
        return pl.ds(pl.multiple_of(tile_index * tile, tile), tile)

    def arrived(ref, sem):
        pltpu.make_async_copy(ref, ref, sem).wait()

    for n, source in enumerate(inputs):
        for r in row_peers:
            for h in range(halves):
                send(
                    source.at[:, lanes(h * rows + r)],
                    by_row.at[n, col, row, :, h * tile : (h + 1) * tile],
                    swap_sem.at[n, 0],
                    {"row": r},
                )
        for c in col_peers:
            for b in range(blocks):
                send(
                    source.at[:, lanes(b * cols + c)],
                    by_col.at[n, row, col, :, b * tile : (b + 1) * tile],
                    swap_sem.at[n, 1],
                    {"col": c},
                )
    for n, source in enumerate(inputs):
        for h in range(halves):
            by_row[n, col, row, :, h * tile : (h + 1) * tile] = source[:, lanes(h * rows + row)]
        for b in range(blocks):
            by_col[n, row, col, :, b * tile : (b + 1) * tile] = source[:, lanes(b * cols + col)]

    kinds = [(n, part) for n in range(2) for part in range(2)]
    axes = ("col", "row")
    held = (by_row, by_col)

    def gathered(n, part, across, along, half=None):
        whole = held[part].at[n, place(axes[part], across, along)]
        if half is None:
            return whole
        size = whole.shape[0] // 2
        return whole.at[pl.ds(half * size, size)]

    def along_ring(n, part, across, along, way, half, sem):
        what = gathered(n, part, across, along, half)
        where = {axes[part]: place(axes[part], 0, way)}
        send(what, what, gather_sem.at[n, part, sem], where)

    def to_core(n, part, across, along, half=None):
        if part == 1:
            what = gathered(n, part, across, along, half)
            send(what, what, gather_core.at[n], {"row": row + 1 - 2 * core})

    def wait_ring(n, part, across, along, half, sem):
        arrived(gathered(n, part, across, along, half), gather_sem.at[n, part, sem])

    for n, part in kinds:
        count = (rows if part == 0 else cols) - 1
        mine = (col if part == 0 else row,)
        arrived(held[part].at[n, mine[0], pl.ds(0, count)], swap_sem.at[n, part])
        along_ring(n, part, 0, 0, 1, None, 0)
        along_ring(n, part, 0, 0, -1, None, 1)
        what = gathered(n, part, 0, 0)
        send(what, what, gather_sem.at[n, part, 2], {axes[part]: place(axes[part], 1, 0)})
        to_core(n, part, 0, 0)
    for n, part in kinds:
        wait_ring(n, part, 0, -1, None, 0)
        along_ring(n, part, 0, -1, 1, 0, 3)
        to_core(n, part, 0, -1)
        wait_ring(n, part, 0, 1, None, 1)
        along_ring(n, part, 0, 1, -1, 1, 4)
        to_core(n, part, 0, 1)
        wait_ring(n, part, 1, 0, None, 2)
        along_ring(n, part, 1, 0, 1, None, 5)
        along_ring(n, part, 1, 0, -1, None, 6)
        to_core(n, part, 1, 0)
    for n, part in kinds:
        wait_ring(n, part, 0, 2, 0, 3)
        to_core(n, part, 0, 2, 0)
        wait_ring(n, part, 0, 2, 1, 4)
        to_core(n, part, 0, 2, 1)
        wait_ring(n, part, 1, -1, None, 5)
        along_ring(n, part, 1, -1, 1, 0, 7)
        to_core(n, part, 1, -1)
        wait_ring(n, part, 1, 1, None, 6)
        along_ring(n, part, 1, 1, -1, 1, 8)
        to_core(n, part, 1, 1)
    for n, part in kinds:
        wait_ring(n, part, 1, 2, 0, 7)
        to_core(n, part, 1, 2, 0)
        wait_ring(n, part, 1, 2, 1, 8)
        to_core(n, part, 1, 2, 1)
    for n in range(2):
        arrived(by_col.at[n, pl.ds(0, rows // 2)], gather_core.at[n])


    def eig_place(across, along):
        return place("row", across, along)

    def psi_place(across, along):
        return place("col", across, along)

    def piece(held, index, half):
        whole = held.at[index]
        if half is None:
            return whole
        size = whole.shape[0] // 2
        return whole.at[pl.ds(half * size, size)]

    def eig_send(across, along, way, half, sem):
        what = piece(eig_cols, eig_place(across, along), half)
        to = eig_place(1, 0) if way is None else eig_place(0, way)
        send(what, what, eig_sem.at[sem], {"row": to, "col": col})

    def eig_core(across, along, half):
        what = piece(eig_cols, eig_place(across, along), half)
        send(what, what, core_sem, {"row": row + 1 - 2 * core, "col": col})

    def eig_wait(across, along, half, sem):
        arrived(piece(eig_cols, eig_place(across, along), half), eig_sem.at[sem])

    def psi_send(across, along, way, half, sem):
        what = piece(psi_rows, psi_place(across, along), half)
        to = psi_place(1, 0) if way is None else psi_place(0, way)
        send(what, what, psi_sem.at[sem], {"row": row, "col": to})

    def psi_wait(across, along, half, sem):
        arrived(piece(psi_rows, psi_place(across, along), half), psi_sem.at[sem])

    depth = rows * by_row.shape[3]

    def row_block(n, c):
        return by_row[n, c].reshape(depth, halves * tile)

    def col_block(n, c):
        return by_col[n, :, c].reshape(depth, blocks * tile)

    def product(left, right):
        return lax.dot_general(
            left, right, (((0,), (0,)), ((), ())), preferred_element_type=jnp.float32
        )

    def add_s(c, carry):
        total_s[...] += product(row_block(0, c), col_block(0, c))
        return carry

    def add_a(c, carry):
        a_ref[...] += product(row_block(0, c), col_block(1, c)) + product(
            row_block(1, c), col_block(0, c)
        )
        return carry

    a_ref[...] = jnp.zeros_like(a_ref)
    lax.fori_loop(0, cols, add_a, 0)
    a_ref[...] = 0.5 * a_ref[...]

    def to_heads(source, target, recv):
        for peer in heads:
            send(source, target, recv, peer)

    @pl.when(col == 0)
    def _():
        for half in range(halves):
            first = a_ref[half * tile : (half + 1) * tile, 0:tile]
            panel_in[row, :, half, :] = jnp.transpose(first)[0 : PB + 1, :]
        mine = panel_in.at[row]
        for peer in around:
            send(mine, mine, panel_sem.at[core], {**peer, "row": head})

        @pl.when(core == 0)
        def _():
            send(mine, mine, panel_sem.at[0], {"row": head})

    above, below = lax.rem(ring + 1, turns), lax.rem(ring + turns - 1, turns)
    half_rows = height // 2

    def part_of(where, k, half):
        first = pl.multiple_of(k * height + half * half_rows, half_rows)
        return a_plane.at[where, pl.ds(first, half_rows)]

    for half in range(2):
        for way, part in ((0, half), (1, 1 - half)):
            send(
                a_ref.at[pl.ds(part * half_rows, half_rows)],
                part_of(ring, core, part),
                ring_sem.at[core, 2 * way + part],
                {**around[way], "row": head},
            )

    own_rows = pl.ds(pl.multiple_of(core * height, height), height)

    @pl.when(core == 0)
    def _():
        send(a_ref, a_plane.at[ring, own_rows], back_sem.at[3], {"row": head})

    @pl.when((core == 1) & (pair == 0))
    def _():
        arrived(panel_in.at[row - core], panel_sem.at[0])

        @pl.when(ring > 0)
        def _():
            arrived(panel_in.at[row], panel_sem.at[1])

        both = panel_in.at[pl.ds(row - core, 2)]
        to_heads(both, both, panel_sem.at[2])

    eig_cols[row] = eig_ref[...]
    psi_rows[col] = psi_ref[...]
    eig_send(0, 0, 1, None, 0)
    eig_send(0, 0, -1, None, 1)
    eig_send(0, 0, None, None, 2)
    eig_core(0, 0, None)
    psi_send(0, 0, None, None, 2)


    spot = lax.broadcasted_iota(jnp.int32, (tiles, tile), 0)
    lane = lax.broadcasted_iota(jnp.int32, (tiles, tile), 1)
    positions = ((spot % halves) * rows + spot // halves) * tile + lane
    slot = lax.broadcasted_iota(jnp.int32, (8, tile), 1)

    @pl.when(core == 1)
    def _():
        a_plane[ring, height : 2 * height, :] = a_ref[...]
        vecs[...] = jnp.zeros_like(vecs)
        images[...] = jnp.zeros_like(images)

        @pl.when(pair == 0)
        def _():
            arrived(panel_in.at[pl.ds(0, rows - 2)], panel_sem.at[2])

        @pl.when(pair > 0)
        def _():
            arrived(panel_in, panel_sem.at[2])

        for r in range(rows):
            panel[:, r * halves : (r + 1) * halves, :] = panel_in[r]
        for k in range(2):
            arrived(part_of(below, k, 0), ring_sem.at[k, 0])
            send(part_of(below, k, 0), part_of(below, k, 0), ring_sem.at[k, 4], around[0])
            arrived(part_of(above, k, 1), ring_sem.at[k, 3])
            send(part_of(above, k, 1), part_of(above, k, 1), ring_sem.at[k, 5], around[1])

    eig_wait(0, -1, None, 0)
    eig_send(0, -1, 1, 0, 3)
    eig_core(0, -1, None)
    eig_wait(0, 1, None, 1)
    eig_send(0, 1, -1, 1, 4)
    eig_core(0, 1, None)
    eig_wait(1, 0, None, 2)
    eig_send(1, 0, 1, None, 5)
    eig_send(1, 0, -1, None, 6)
    eig_core(1, 0, None)
    psi_send(0, 0, 1, None, 0)
    psi_send(0, 0, -1, None, 1)
    psi_wait(1, 0, None, 2)
    psi_send(1, 0, 1, None, 5)
    psi_send(1, 0, -1, None, 6)
    across = lax.rem(ring + 2, turns)

    def background(step):
        @pl.when(step == 0)
        def _():
            eig_wait(0, 2, 0, 3)
            eig_core(0, 2, 0)
            eig_wait(0, 2, 1, 4)
            eig_core(0, 2, 1)
            eig_wait(1, -1, None, 5)
            eig_send(1, -1, 1, 0, 7)
            eig_core(1, -1, None)
            eig_wait(1, 1, None, 6)
            eig_send(1, 1, -1, 1, 8)
            eig_core(1, 1, None)

        @pl.when(step == 2)
        def _():
            eig_wait(1, 2, 0, 7)
            eig_core(1, 2, 0)
            eig_wait(1, 2, 1, 8)
            eig_core(1, 2, 1)
            psi_wait(0, -1, None, 0)
            psi_send(0, -1, 1, 0, 3)
            psi_wait(0, 1, None, 1)
            psi_send(0, 1, -1, 1, 4)

        @pl.when(step == 3)
        def _():
            total_s[...] = jnp.zeros_like(total_s)
            lax.fori_loop(0, cols, add_s, 0)

        @pl.when(step == 5)
        def _():
            scale = 1.0 / (rows * cols * psi_ref.shape[0])
            for b in range(blocks):
                corr_ref[pl.ds(b, height, stride=blocks), :] = scale * total_s[
                    :, b * tile : (b + 1) * tile
                ]

        @pl.when(step == 4)
        def _():
            psi_wait(1, -1, None, 5)
            psi_send(1, -1, 1, 0, 7)
            psi_wait(1, 1, None, 6)
            psi_send(1, 1, -1, 1, 8)

        @pl.when(step == 6)
        def _():
            for half in range(2):
                psi_wait(0, 2, half, 3 + half)
                psi_wait(1, 2, half, 7 + half)
            arrived(eig_cols.at[pl.ds(0, rows // 2)], core_sem)
            rotated[...] = jnp.zeros_like(rotated)

        @pl.when((step >= PB // 2 - 1) & (step < PB - 1))
        def _():
            per = rows // (PB // 2)
            for k in range(per):
                r = (step - PB // 2 + 1) * per + k
                left = [
                    psi_rows[:, :, pl.ds(pl.multiple_of((h * rows + r) * tile, tile), tile)]
                    for h in range(halves)
                ]
                left = jnp.concatenate([x.reshape(-1, tile) for x in left], axis=1)
                rotated[...] += jnp.dot(left, eig_cols[r], preferred_element_type=jnp.float32)

        @pl.when(step == PB - 1)
        def _():
            depth = rotated.shape[0]
            for b in range(blocks):
                rotated_tiles[pl.ds(b, depth, stride=blocks), :] = rotated[
                    :, b * tile : (b + 1) * tile
                ]
            rotated_ref[...] = rotated_tiles[...].astype(rotated_ref.dtype)

    def total(x):
        return jnp.sum(x, axis=(0, 1), keepdims=True)

    def totals(x):
        return jnp.sum(x, axis=(1, 2), keepdims=True)

    def reflector(column, step):
        at = total(jnp.where(positions == step, column, 0.0))
        pivot = total(jnp.where(positions == step + 1, column, 0.0))
        under = positions > step + 1
        tail = total(jnp.where(under, column * column, 0.0))
        length = jnp.sqrt(pivot * pivot + tail)
        beta = jnp.where(pivot >= 0.0, -length, length)
        tau = (beta - pivot) / beta
        scale = 1.0 / (pivot - beta)
        vector = jnp.where(positions == step + 1, 1.0, jnp.where(under, column * scale, 0.0))
        return at, beta, tau, scale, vector

    def advance(step, carry):
        column, diagonal, offdiag = carry
        vec[...] = jnp.where(positions > step + 1, column, 0.0)
        spread = []
        for y in range(turns):
            for b in range(blocks):
                t = b * cols + pair * turns + y
                e = lax.rem(t, rows) * halves + lax.div(t, rows)
                spread.append(jnp.broadcast_to(vec[pl.ds(e, 1), :], (8, tile)))

        def band(group, _):
            at_rows = pl.ds(pl.multiple_of(group * 8, 8), 8)
            sums = [jnp.zeros((8, tile), jnp.float32) for _ in range(4)]
            for y in range(turns):
                for b in range(blocks):
                    block = a_plane[y, at_rows, b * tile : (b + 1) * tile]
                    sums[b] = sums[b] + block * spread[y * blocks + b]
            lanes_sum[at_rows, :] = (sums[0] + sums[1]) + (sums[2] + sums[3])
            return 0

        lax.fori_loop(0, 2 * height // 8, band, 0, unroll=16)
        ones = jnp.ones((16, tile), jnp.bfloat16)
        product = jnp.zeros((16, 2 * height), jnp.float32)
        for piece in split_three(lanes_sum[...]):
            product = product + lax.dot_general(
                ones, piece, (((1,), (1,)), ((), ())), preferred_element_type=jnp.float32
            )
        for q in range(2 * halves):
            parts_out[step, q : q + 1, :] = product[0:1, q * tile : (q + 1) * tile]
        mine = pair * (rows // 2) + chip
        to_heads(parts_out.at[step], parts_in.at[step, mine], parts_sem.at[step])
        parts_in[step, mine] = parts_out[step]
        at, beta, tau, scale, vector = reflector(column, step)
        diagonal = jnp.where(slot == step, at, diagonal)
        offdiag = jnp.where(slot == step, beta, offdiag)
        background(step)
        by_vecs = totals(vecs[...] * vector[None])
        by_images = totals(images[...] * vector[None])
        known = jnp.sum(vecs[...] * by_images + images[...] * by_vecs, axis=0)
        following = jnp.minimum(step + 1, PB - 1)
        here = positions == following
        head_v = totals(jnp.where(here[None], vecs[...], 0.0))
        head_w = totals(jnp.where(here[None], images[...], 0.0))
        ahead = panel[following] - jnp.sum(vecs[...] * head_w + images[...] * head_v, axis=0)
        vecs[step] = vector
        send(vecs.at[step], vecs.at[step], back_sem.at[0], {"row": row - core})
        lead_v = total(jnp.where(here, vector, 0.0))
        half_tau = 0.5 * tau * tau
        base = panel[step + 1] - known
        arrived(parts_in.at[step, pl.ds(0, rows - 1)], parts_sem.at[step])
        for m in range(rows // 2):
            whole[m * 2 * halves : (m + 1) * 2 * halves, :] = (
                parts_in[step, m] + parts_in[step, rows // 2 + m]
            )
        change = scale * whole[...] + base
        along = half_tau * total(change * vector)
        lead_w = tau * total(jnp.where(here, change, 0.0)) - along * lead_v
        image = tau * change - along * vector
        images[step] = image
        send(images.at[step], images.at[step], back_sem.at[1], {"row": row - core})
        column = ahead - vector * lead_w - image * lead_v
        return column, diagonal, offdiag

    @pl.when(core == 1)
    def _():
        for k in range(2):
            arrived(part_of(below, k, 1), ring_sem.at[k, 1])
            arrived(part_of(above, k, 0), ring_sem.at[k, 2])
            arrived(part_of(across, k, 0), ring_sem.at[k, 4])
            arrived(part_of(across, k, 1), ring_sem.at[k, 5])
        arrived(a_plane.at[ring, pl.ds(0, height)], back_sem.at[3])
        nothing = jnp.zeros((8, tile), jnp.float32)
        _, diagonal, offdiag = lax.fori_loop(0, PB, advance, (panel[0], nothing, nothing))
        ends[0] = diagonal
        ends[1] = offdiag
        send(ends, ends, back_sem.at[2], {"row": row - core})

    @pl.when(core == 0)
    def _():
        def wait_step(step, carry):
            background(step)
            return carry

        lax.fori_loop(0, PB, wait_step, 0)
        arrived(vecs, back_sem.at[0])
        arrived(images, back_sem.at[1])
        arrived(ends, back_sem.at[2])

    diag_ref[...] = ends[0, 0:1, 0:PB]
    off_ref[...] = ends[1, 0:1, 0:PB]
    left_v = [vecs[:, pl.ds(halves * row + h, 1), :].reshape(PB, tile) for h in range(halves)]
    left_w = [images[:, pl.ds(halves * row + h, 1), :].reshape(PB, tile) for h in range(halves)]
    for b in range(blocks):
        t = b * cols + col
        e = (t % rows) * halves + t // rows
        right_v = vecs[:, pl.ds(e, 1), :].reshape(PB, tile)
        right_w = images[:, pl.ds(e, 1), :].reshape(PB, tile)
        for h in range(halves):
            change = lax.dot_general(
                jnp.concatenate([left_v[h], left_w[h]], axis=0),
                jnp.concatenate([right_w, right_v], axis=0),
                (((0,), (0,)), ((), ())),
                precision=lax.Precision.HIGHEST,
                preferred_element_type=jnp.float32,
            )
            block = a_ref[h * tile : (h + 1) * tile, b * tile : (b + 1) * tile]
            updated_ref[pl.ds(h * tile * blocks + b, tile, stride=blocks), :] = block - change


    def sent(ref):
        pltpu.make_async_copy(ref, ref, send_sem).wait()

    @pl.when(col == 0)
    def _():
        sent(panel_in.at[pl.ds(0, len(around))])

    for _ in range(2):
        sent(a_ref)

    @pl.when(core == 0)
    def _():
        sent(a_ref)

        @pl.when(col == 0)
        def _():
            sent(panel_in.at[0])

    @pl.when(core == 1)
    def _():
        @pl.when(pair == 0)
        def _():
            sent(panel_in)
            sent(panel_in.at[pl.ds(0, rows - 2)])

        for _ in range(2):
            sent(a_ref)
        sent(vecs)
        sent(images)
        sent(ends)

    sent(eig_cols.at[pl.ds(0, 7)])
    sent(eig_cols.at[pl.ds(0, rows // 2)])
    sent(psi_rows.at[pl.ds(0, 7)])

    def drain(step, carry):
        sent(parts_in.at[step, pl.ds(0, rows - 1)])
        return carry

    @pl.when(core == 1)
    def _():
        lax.fori_loop(0, PB, drain, 0)

    for n in range(2):
        sent(by_row.at[n, 0, pl.ds(0, rows - 1)])
        sent(by_col.at[n, 0, pl.ds(0, cols - 1)])
        sent(by_row.at[n, pl.ds(0, 7)])
        sent(by_col.at[n, pl.ds(0, 7)])
        sent(by_col.at[n, pl.ds(0, rows // 2)])


def reduce_and_rotate(psi, hpsi, eigvec, rows, cols):
    height, width = eigvec.shape
    tile = 128
    halves = height // tile
    tiles = rows * halves
    depth = cols * psi.shape[0]
    vmem = pl.BlockSpec(memory_space=pltpu.VMEM)
    block = pltpu.VMEM((height, width), jnp.float32)
    vectors = pltpu.VMEM((PB, tiles, tile), jnp.float32)
    laid = jax.ShapeDtypeStruct((height * width // tile, tile), jnp.float32)
    return pl.pallas_call(
        whole_kernel,
        out_shape=(
            laid,
            laid,
            jax.ShapeDtypeStruct((1, PB), jnp.float32),
            jax.ShapeDtypeStruct((1, PB), jnp.float32),
            jax.ShapeDtypeStruct((depth * width // tile, tile), psi.dtype),
        ),
        in_specs=[vmem] * 3,
        out_specs=(vmem,) * 5,
        scratch_shapes=[
            pltpu.VMEM((2, cols, rows, psi.shape[0], height), psi.dtype),
            pltpu.VMEM((2, rows, cols, psi.shape[0], width), psi.dtype),
            block,
            block,
            pltpu.VMEM((cols, *psi.shape), psi.dtype),
            pltpu.VMEM((rows, *eigvec.shape), eigvec.dtype),
            pltpu.VMEM((depth, width), jnp.float32),
            pltpu.VMEM((depth * width // tile, tile), jnp.float32),
            pltpu.VMEM((cols // 2, 2 * height, width), jnp.float32),
            pltpu.VMEM((rows, PB + 1, halves, tile), jnp.float32),
            pltpu.VMEM((PB + 1, tiles, tile), jnp.float32),
            vectors,
            vectors,
            pltpu.VMEM((tiles, tile), jnp.float32),
            pltpu.VMEM((2 * height, tile), jnp.float32),
            pltpu.VMEM((PB, 2 * halves, tile), jnp.float32),
            pltpu.VMEM((PB, rows, 2 * halves, tile), jnp.float32),
            pltpu.VMEM((tiles, tile), jnp.float32),
            pltpu.VMEM((2, 8, tile), jnp.float32),
            pltpu.SemaphoreType.DMA,
            pltpu.SemaphoreType.DMA((2, 2)),
            pltpu.SemaphoreType.DMA((2, 2, 9)),
            pltpu.SemaphoreType.DMA((2,)),
            pltpu.SemaphoreType.DMA((2, 6)),
            pltpu.SemaphoreType.DMA((3,)),
            pltpu.SemaphoreType.DMA((PB,)),
            pltpu.SemaphoreType.DMA((9,)),
            pltpu.SemaphoreType.DMA,
            pltpu.SemaphoreType.DMA((9,)),
            pltpu.SemaphoreType.DMA((4,)),
        ],
        compiler_params=pltpu.CompilerParams(
            collective_id=0, has_side_effects=True, vmem_limit_bytes=56 * 1024 * 1024
        ),
        name="whole",
    )(psi, hpsi, eigvec)


def on_device(psi, hpsi, eigvec):
    row_tiles, _, tile_size, col_tiles = eigvec.shape[:4]
    correlation, updated, diagonal, offdiag, rotated = reduce_and_rotate(
        psi,
        hpsi,
        eigvec.reshape(row_tiles * tile_size, col_tiles * tile_size),
        lax.axis_size("row"),
        lax.axis_size("col"),
    )
    tile_shape = (row_tiles, 1, tile_size, col_tiles, 1, tile_size)
    return (
        correlation.reshape(tile_shape),
        updated.reshape(tile_shape),
        diagonal.reshape(PB),
        offdiag.reshape(PB),
        rotated.reshape(-1, col_tiles, 1, tile_size),
    )


def solution(mesh):
    return jax.shard_map(
        on_device,
        mesh=mesh,
        in_specs=(
            P(("row", "col"), None),
            P(("row", "col"), None),
            P(None, "row", None, None, "col", None),
        ),
        out_specs=(
            P(None, "row", None, None, "col", None),
            P(None, "row", None, None, "col", None),
            P(),
            P(),
            P("row", None, "col", None),
        ),
        check_vma=False,
    )
```

```python
import jax
import jax.numpy as jnp
from jax import lax
from jax.experimental import pallas as pl
from jax.experimental.pallas import tpu as pltpu
from jax.sharding import PartitionSpec as P

PB = 16
MESH = pl.DeviceIdType.MESH


def split_three(x):
    high = x.astype(jnp.bfloat16)
    rest = x - high.astype(jnp.float32)
    mid = rest.astype(jnp.bfloat16)
    low = (rest - mid.astype(jnp.float32)).astype(jnp.bfloat16)
    return high, mid, low


def lattice(row, col):
    pair = {"row": lax.div(row, 8), "col": lax.div(col, 4)}
    ring = {"row": lax.rem(lax.div(row, 2), 4), "col": lax.rem(col, 4)}
    return pair, ring


def whole_kernel(
    psi_ref,
    hpsi_ref,
    eig_ref,
    corr_ref,
    updated_ref,
    diag_ref,
    off_ref,
    rotated_ref,
    by_row,
    by_col,
    total_s,
    a_ref,
    psi_rows,
    eig_cols,
    rotated,
    rotated_tiles,
    a_plane,
    panel_in,
    panel,
    vecs,
    images,
    vec,
    lanes_sum,
    parts_out,
    parts_in,
    whole,
    ends,
    send_sem,
    swap_sem,
    gather_sem,
    gather_core,
    ring_sem,
    panel_sem,
    parts_sem,
    eig_sem,
    core_sem,
    psi_sem,
    back_sem,
):
    rows = lax.axis_size("row")
    cols = lax.axis_size("col")
    row = lax.axis_index("row")
    col = lax.axis_index("col")
    tile = 128
    height, width = a_ref.shape
    halves, blocks = height // tile, width // tile
    tiles = rows * halves
    turns = cols // 2
    pairs, rings = lattice(row, col)
    pair, ring = pairs["col"], rings["col"]
    inputs = (psi_ref, hpsi_ref)
    core = lax.rem(row, 2)

    def place(axis, across, along):
        p = lax.rem(pairs[axis] + across, 2)
        q = lax.rem(rings[axis] + along + 4, 4)
        return p * 8 + q * 2 + core if axis == "row" else p * 4 + q

    order = sorted(
        ((d, e) for d in range(rows) for e in range(2) if d + e > 0),
        key=lambda de: -min(de[0], rows - de[0]) - 4 * de[1],
    )
    peers = [
        {"row": lax.rem(row + d, rows), "col": lax.rem(pair + e, 2) * turns + ring}
        for d, e in order
    ]
    around = [{"row": row, "col": pair * turns + lax.rem(ring + d, turns)} for d in (1, 3, 2)]
    beyond = [
        {"row": row, "col": (1 - pair) * turns + lax.rem(ring + d, turns)} for d in (1, 3, 2)
    ]
    row_order = sorted(range(1, rows), key=lambda d: -min(d, rows - d))
    row_peers = [lax.rem(row + d, rows) for d in row_order]
    col_peers = [lax.rem(col + d, cols) for d in range(1, cols)]
    chip = lax.div(row, 2)
    head = row - core + 1
    hops = {(0, 0): 0, (1, 0): 1, (0, 1): 2, (1, 1): 1}
    steps = [(x, z, e) for x in range(2) for z in range(4) for e in range(2) if x + z + e > 0]
    heads = [
        {
            "row": lax.rem(pairs["row"] + x, 2) * 8 + lax.rem(rings["row"] + z, 4) * 2 + 1,
            "col": lax.rem(pair + e, 2) * turns + ring,
        }
        for x, z, e in sorted(steps, key=lambda q: -hops[q[0], q[2]] - min(q[1], 4 - q[1]))
    ]
    aside = [{**peer, "row": row + 1 - 2 * core} for peer in around]
    greeted = peers + around + beyond + aside
    barrier = pltpu.get_barrier_semaphore()
    for peer in greeted:
        pl.semaphore_signal(barrier, inc=1, device_id=peer, device_id_type=MESH)
    pl.semaphore_wait(barrier, len(greeted))

    def send(source, target, sem, where):
        pltpu.make_async_remote_copy(
            src_ref=source,
            dst_ref=target,
            send_sem=send_sem,
            recv_sem=sem,
            device_id={"row": row, "col": col, **where},
            device_id_type=MESH,
        ).start()

    def lanes(tile_index):
        return pl.ds(pl.multiple_of(tile_index * tile, tile), tile)

    def arrived(ref, sem):
        pltpu.make_async_copy(ref, ref, sem).wait()

    for n, source in enumerate(inputs):
        for r in row_peers:
            for h in range(halves):
                send(
                    source.at[:, lanes(h * rows + r)],
                    by_row.at[n, col, row, :, h * tile : (h + 1) * tile],
                    swap_sem.at[n, 0],
                    {"row": r},
                )
        for c in col_peers:
            for b in range(blocks):
                send(
                    source.at[:, lanes(b * cols + c)],
                    by_col.at[n, row, col, :, b * tile : (b + 1) * tile],
                    swap_sem.at[n, 1],
                    {"col": c},
                )
    for n, source in enumerate(inputs):
        for h in range(halves):
            by_row[n, col, row, :, h * tile : (h + 1) * tile] = source[:, lanes(h * rows + row)]
        for b in range(blocks):
            by_col[n, row, col, :, b * tile : (b + 1) * tile] = source[:, lanes(b * cols + col)]

    kinds = [(n, part) for n in range(2) for part in range(2)]
    axes = ("col", "row")
    held = (by_row, by_col)

    def gathered(n, part, across, along, half=None):
        whole = held[part].at[n, place(axes[part], across, along)]
        if half is None:
            return whole
        size = whole.shape[0] // 2
        return whole.at[pl.ds(half * size, size)]

    def along_ring(n, part, across, along, way, half, sem):
        what = gathered(n, part, across, along, half)
        where = {axes[part]: place(axes[part], 0, way)}
        send(what, what, gather_sem.at[n, part, sem], where)

    def to_core(n, part, across, along, half=None):
        if part == 1:
            what = gathered(n, part, across, along, half)
            send(what, what, gather_core.at[n], {"row": row + 1 - 2 * core})

    def wait_ring(n, part, across, along, half, sem):
        arrived(gathered(n, part, across, along, half), gather_sem.at[n, part, sem])

    for n, part in kinds:
        count = (rows if part == 0 else cols) - 1
        mine = (col if part == 0 else row,)
        arrived(held[part].at[n, mine[0], pl.ds(0, count)], swap_sem.at[n, part])
        along_ring(n, part, 0, 0, 1, None, 0)
        along_ring(n, part, 0, 0, -1, None, 1)
        what = gathered(n, part, 0, 0)
        send(what, what, gather_sem.at[n, part, 2], {axes[part]: place(axes[part], 1, 0)})
        to_core(n, part, 0, 0)
    for n, part in kinds:
        wait_ring(n, part, 0, -1, None, 0)
        along_ring(n, part, 0, -1, 1, 0, 3)
        to_core(n, part, 0, -1)
        wait_ring(n, part, 0, 1, None, 1)
        along_ring(n, part, 0, 1, -1, 1, 4)
        to_core(n, part, 0, 1)
        wait_ring(n, part, 1, 0, None, 2)
        along_ring(n, part, 1, 0, 1, None, 5)
        along_ring(n, part, 1, 0, -1, None, 6)
        to_core(n, part, 1, 0)
    for n, part in kinds:
        wait_ring(n, part, 0, 2, 0, 3)
        to_core(n, part, 0, 2, 0)
        wait_ring(n, part, 0, 2, 1, 4)
        to_core(n, part, 0, 2, 1)
        wait_ring(n, part, 1, -1, None, 5)
        along_ring(n, part, 1, -1, 1, 0, 7)
        to_core(n, part, 1, -1)
        wait_ring(n, part, 1, 1, None, 6)
        along_ring(n, part, 1, 1, -1, 1, 8)
        to_core(n, part, 1, 1)
    for n, part in kinds:
        wait_ring(n, part, 1, 2, 0, 7)
        to_core(n, part, 1, 2, 0)
        wait_ring(n, part, 1, 2, 1, 8)
        to_core(n, part, 1, 2, 1)
    for n in range(2):
        arrived(by_col.at[n, pl.ds(0, rows // 2)], gather_core.at[n])


    def eig_place(across, along):
        return place("row", across, along)

    def psi_place(across, along):
        return place("col", across, along)

    def piece(held, index, half):
        whole = held.at[index]
        if half is None:
            return whole
        size = whole.shape[0] // 2
        return whole.at[pl.ds(half * size, size)]

    def eig_send(across, along, way, half, sem):
        what = piece(eig_cols, eig_place(across, along), half)
        to = eig_place(1, 0) if way is None else eig_place(0, way)
        send(what, what, eig_sem.at[sem], {"row": to, "col": col})

    def eig_core(across, along, half):
        what = piece(eig_cols, eig_place(across, along), half)
        send(what, what, core_sem, {"row": row + 1 - 2 * core, "col": col})

    def eig_wait(across, along, half, sem):
        arrived(piece(eig_cols, eig_place(across, along), half), eig_sem.at[sem])

    def psi_send(across, along, way, half, sem):
        what = piece(psi_rows, psi_place(across, along), half)
        to = psi_place(1, 0) if way is None else psi_place(0, way)
        send(what, what, psi_sem.at[sem], {"row": row, "col": to})

    def psi_wait(across, along, half, sem):
        arrived(piece(psi_rows, psi_place(across, along), half), psi_sem.at[sem])

    depth = rows * by_row.shape[3]

    def row_block(n, c):
        return by_row[n, c].reshape(depth, halves * tile)

    def col_block(n, c):
        return by_col[n, :, c].reshape(depth, blocks * tile)

    def product(left, right):
        return lax.dot_general(
            left, right, (((0,), (0,)), ((), ())), preferred_element_type=jnp.float32
        )

    def add_s(c, carry):
        total_s[...] += product(row_block(0, c), col_block(0, c))
        return carry

    def add_a(c, carry):
        a_ref[...] += product(row_block(0, c), col_block(1, c)) + product(
            row_block(1, c), col_block(0, c)
        )
        return carry

    a_ref[...] = jnp.zeros_like(a_ref)
    lax.fori_loop(0, cols, add_a, 0)
    a_ref[...] = 0.5 * a_ref[...]

    def to_heads(source, target, recv):
        for peer in heads:
            send(source, target, recv, peer)

    @pl.when(col == 0)
    def _():
        for half in range(halves):
            first = a_ref[half * tile : (half + 1) * tile, 0:tile]
            panel_in[row, :, half, :] = jnp.transpose(first)[0 : PB + 1, :]
        mine = panel_in.at[row]
        for peer in around:
            send(mine, mine, panel_sem.at[core], {**peer, "row": head})

        @pl.when(core == 0)
        def _():
            send(mine, mine, panel_sem.at[0], {"row": head})

    above, below = lax.rem(ring + 1, turns), lax.rem(ring + turns - 1, turns)
    half_rows = height // 2

    def part_of(where, k, half):
        first = pl.multiple_of(k * height + half * half_rows, half_rows)
        return a_plane.at[where, pl.ds(first, half_rows)]

    for half in range(2):
        for way, part in ((0, half), (1, 1 - half)):
            send(
                a_ref.at[pl.ds(part * half_rows, half_rows)],
                part_of(ring, core, part),
                ring_sem.at[core, 2 * way + part],
                {**around[way], "row": head},
            )

    own_rows = pl.ds(pl.multiple_of(core * height, height), height)

    @pl.when(core == 0)
    def _():
        send(a_ref, a_plane.at[ring, own_rows], back_sem.at[3], {"row": head})

    @pl.when((core == 1) & (pair == 0))
    def _():
        arrived(panel_in.at[row - core], panel_sem.at[0])

        @pl.when(ring > 0)
        def _():
            arrived(panel_in.at[row], panel_sem.at[1])

        both = panel_in.at[pl.ds(row - core, 2)]
        to_heads(both, both, panel_sem.at[2])

    eig_cols[row] = eig_ref[...]
    psi_rows[col] = psi_ref[...]
    eig_send(0, 0, 1, None, 0)
    eig_send(0, 0, -1, None, 1)
    eig_send(0, 0, None, None, 2)
    eig_core(0, 0, None)
    psi_send(0, 0, None, None, 2)


    spot = lax.broadcasted_iota(jnp.int32, (tiles, tile), 0)
    lane = lax.broadcasted_iota(jnp.int32, (tiles, tile), 1)
    positions = ((spot % halves) * rows + spot // halves) * tile + lane
    slot = lax.broadcasted_iota(jnp.int32, (8, tile), 1)

    @pl.when(core == 1)
    def _():
        a_plane[ring, height : 2 * height, :] = a_ref[...]
        vecs[...] = jnp.zeros_like(vecs)
        images[...] = jnp.zeros_like(images)

        @pl.when(pair == 0)
        def _():
            arrived(panel_in.at[pl.ds(0, rows - 2)], panel_sem.at[2])

        @pl.when(pair > 0)
        def _():
            arrived(panel_in, panel_sem.at[2])

        for r in range(rows):
            panel[:, r * halves : (r + 1) * halves, :] = panel_in[r]
        for k in range(2):
            arrived(part_of(below, k, 0), ring_sem.at[k, 0])
            send(part_of(below, k, 0), part_of(below, k, 0), ring_sem.at[k, 4], around[0])
            arrived(part_of(above, k, 1), ring_sem.at[k, 3])
            send(part_of(above, k, 1), part_of(above, k, 1), ring_sem.at[k, 5], around[1])

    eig_wait(0, -1, None, 0)
    eig_send(0, -1, 1, 0, 3)
    eig_core(0, -1, None)
    eig_wait(0, 1, None, 1)
    eig_send(0, 1, -1, 1, 4)
    eig_core(0, 1, None)
    eig_wait(1, 0, None, 2)
    eig_send(1, 0, 1, None, 5)
    eig_send(1, 0, -1, None, 6)
    eig_core(1, 0, None)
    psi_send(0, 0, 1, None, 0)
    psi_send(0, 0, -1, None, 1)
    psi_wait(1, 0, None, 2)
    psi_send(1, 0, 1, None, 5)
    psi_send(1, 0, -1, None, 6)
    across = lax.rem(ring + 2, turns)

    def background(step):
        @pl.when(step == 0)
        def _():
            eig_wait(0, 2, 0, 3)
            eig_core(0, 2, 0)
            eig_wait(0, 2, 1, 4)
            eig_core(0, 2, 1)
            eig_wait(1, -1, None, 5)
            eig_send(1, -1, 1, 0, 7)
            eig_core(1, -1, None)
            eig_wait(1, 1, None, 6)
            eig_send(1, 1, -1, 1, 8)
            eig_core(1, 1, None)

        @pl.when(step == 2)
        def _():
            eig_wait(1, 2, 0, 7)
            eig_core(1, 2, 0)
            eig_wait(1, 2, 1, 8)
            eig_core(1, 2, 1)
            psi_wait(0, -1, None, 0)
            psi_send(0, -1, 1, 0, 3)
            psi_wait(0, 1, None, 1)
            psi_send(0, 1, -1, 1, 4)

        @pl.when(step == 3)
        def _():
            total_s[...] = jnp.zeros_like(total_s)
            lax.fori_loop(0, cols, add_s, 0)

        @pl.when(step == 5)
        def _():
            scale = 1.0 / (rows * cols * psi_ref.shape[0])
            for b in range(blocks):
                corr_ref[pl.ds(b, height, stride=blocks), :] = scale * total_s[
                    :, b * tile : (b + 1) * tile
                ]

        @pl.when(step == 4)
        def _():
            psi_wait(1, -1, None, 5)
            psi_send(1, -1, 1, 0, 7)
            psi_wait(1, 1, None, 6)
            psi_send(1, 1, -1, 1, 8)

        @pl.when(step == 6)
        def _():
            for half in range(2):
                psi_wait(0, 2, half, 3 + half)
                psi_wait(1, 2, half, 7 + half)
            arrived(eig_cols.at[pl.ds(0, rows // 2)], core_sem)
            rotated[...] = jnp.zeros_like(rotated)

        @pl.when((step >= PB // 2 - 1) & (step < PB - 1))
        def _():
            per = rows // (PB // 2)
            for k in range(per):
                r = (step - PB // 2 + 1) * per + k
                left = [
                    psi_rows[:, :, pl.ds(pl.multiple_of((h * rows + r) * tile, tile), tile)]
                    for h in range(halves)
                ]
                left = jnp.concatenate([x.reshape(-1, tile) for x in left], axis=1)
                rotated[...] += jnp.dot(left, eig_cols[r], preferred_element_type=jnp.float32)

        @pl.when(step == PB - 1)
        def _():
            depth = rotated.shape[0]
            for b in range(blocks):
                rotated_tiles[pl.ds(b, depth, stride=blocks), :] = rotated[
                    :, b * tile : (b + 1) * tile
                ]
            rotated_ref[...] = rotated_tiles[...].astype(rotated_ref.dtype)

    def total(x):
        return jnp.sum(x, axis=(0, 1), keepdims=True)

    def totals(x):
        return jnp.sum(x, axis=(1, 2), keepdims=True)

    def reflector(column, step):
        at = total(jnp.where(positions == step, column, 0.0))
        pivot = total(jnp.where(positions == step + 1, column, 0.0))
        under = positions > step + 1
        tail = total(jnp.where(under, column * column, 0.0))
        length = jnp.sqrt(pivot * pivot + tail)
        beta = jnp.where(pivot >= 0.0, -length, length)
        tau = (beta - pivot) / beta
        scale = 1.0 / (pivot - beta)
        vector = jnp.where(positions == step + 1, 1.0, jnp.where(under, column * scale, 0.0))
        return at, beta, tau, scale, vector

    def advance(step, carry):
        column, diagonal, offdiag = carry
        vec[...] = jnp.where(positions > step + 1, column, 0.0)
        spread = []
        for y in range(turns):
            for b in range(blocks):
                t = b * cols + pair * turns + y
                e = lax.rem(t, rows) * halves + lax.div(t, rows)
                spread.append(jnp.broadcast_to(vec[pl.ds(e, 1), :], (8, tile)))

        def band(group, _):
            at_rows = pl.ds(pl.multiple_of(group * 8, 8), 8)
            sums = [jnp.zeros((8, tile), jnp.float32) for _ in range(4)]
            for y in range(turns):
                for b in range(blocks):
                    block = a_plane[y, at_rows, b * tile : (b + 1) * tile]
                    sums[b] = sums[b] + block * spread[y * blocks + b]
            lanes_sum[at_rows, :] = (sums[0] + sums[1]) + (sums[2] + sums[3])
            return 0

        ones = jnp.ones((16, tile), jnp.bfloat16)
        groups = height // 8
        for k in range(2):
            lax.fori_loop(k * groups, (k + 1) * groups, band, 0, unroll=groups)
            product = jnp.zeros((16, height), jnp.float32)
            for piece in split_three(lanes_sum[k * height : (k + 1) * height, :]):
                product = product + lax.dot_general(
                    ones, piece, (((1,), (1,)), ((), ())), preferred_element_type=jnp.float32
                )
            for half in range(halves):
                q = k * halves + half
                parts_out[step, q : q + 1, :] = product[0:1, half * tile : (half + 1) * tile]
        mine = pair * (rows // 2) + chip
        to_heads(parts_out.at[step], parts_in.at[step, mine], parts_sem.at[step])
        parts_in[step, mine] = parts_out[step]
        at, beta, tau, scale, vector = reflector(column, step)
        diagonal = jnp.where(slot == step, at, diagonal)
        offdiag = jnp.where(slot == step, beta, offdiag)
        background(step)
        by_vecs = totals(vecs[...] * vector[None])
        by_images = totals(images[...] * vector[None])
        known = jnp.sum(vecs[...] * by_images + images[...] * by_vecs, axis=0)
        following = jnp.minimum(step + 1, PB - 1)
        here = positions == following
        head_v = totals(jnp.where(here[None], vecs[...], 0.0))
        head_w = totals(jnp.where(here[None], images[...], 0.0))
        ahead = panel[following] - jnp.sum(vecs[...] * head_w + images[...] * head_v, axis=0)
        vecs[step] = vector
        send(vecs.at[step], vecs.at[step], back_sem.at[0], {"row": row - core})
        lead_v = total(jnp.where(here, vector, 0.0))
        half_tau = 0.5 * tau * tau
        base = panel[step + 1] - known
        arrived(parts_in.at[step, pl.ds(0, rows - 1)], parts_sem.at[step])
        for m in range(rows // 2):
            whole[m * 2 * halves : (m + 1) * 2 * halves, :] = (
                parts_in[step, m] + parts_in[step, rows // 2 + m]
            )
        change = scale * whole[...] + base
        along = half_tau * total(change * vector)
        lead_w = tau * total(jnp.where(here, change, 0.0)) - along * lead_v
        image = tau * change - along * vector
        images[step] = image
        send(images.at[step], images.at[step], back_sem.at[1], {"row": row - core})
        column = ahead - vector * lead_w - image * lead_v
        return column, diagonal, offdiag

    @pl.when(core == 1)
    def _():
        for k in range(2):
            arrived(part_of(below, k, 1), ring_sem.at[k, 1])
            arrived(part_of(above, k, 0), ring_sem.at[k, 2])
            arrived(part_of(across, k, 0), ring_sem.at[k, 4])
            arrived(part_of(across, k, 1), ring_sem.at[k, 5])
        arrived(a_plane.at[ring, pl.ds(0, height)], back_sem.at[3])
        nothing = jnp.zeros((8, tile), jnp.float32)
        _, diagonal, offdiag = lax.fori_loop(0, PB, advance, (panel[0], nothing, nothing))
        ends[0] = diagonal
        ends[1] = offdiag
        send(ends, ends, back_sem.at[2], {"row": row - core})

    @pl.when(core == 0)
    def _():
        def wait_step(step, carry):
            background(step)
            return carry

        lax.fori_loop(0, PB, wait_step, 0)
        arrived(vecs, back_sem.at[0])
        arrived(images, back_sem.at[1])
        arrived(ends, back_sem.at[2])

    diag_ref[...] = ends[0, 0:1, 0:PB]
    off_ref[...] = ends[1, 0:1, 0:PB]
    left_v = [vecs[:, pl.ds(halves * row + h, 1), :].reshape(PB, tile) for h in range(halves)]
    left_w = [images[:, pl.ds(halves * row + h, 1), :].reshape(PB, tile) for h in range(halves)]
    for b in range(blocks):
        t = b * cols + col
        e = (t % rows) * halves + t // rows
        right_v = vecs[:, pl.ds(e, 1), :].reshape(PB, tile)
        right_w = images[:, pl.ds(e, 1), :].reshape(PB, tile)
        for h in range(halves):
            change = lax.dot_general(
                jnp.concatenate([left_v[h], left_w[h]], axis=0),
                jnp.concatenate([right_w, right_v], axis=0),
                (((0,), (0,)), ((), ())),
                precision=lax.Precision.HIGHEST,
                preferred_element_type=jnp.float32,
            )
            block = a_ref[h * tile : (h + 1) * tile, b * tile : (b + 1) * tile]
            updated_ref[pl.ds(h * tile * blocks + b, tile, stride=blocks), :] = block - change


    def sent(ref):
        pltpu.make_async_copy(ref, ref, send_sem).wait()

    @pl.when(col == 0)
    def _():
        sent(panel_in.at[pl.ds(0, len(around))])

    for _ in range(2):
        sent(a_ref)

    @pl.when(core == 0)
    def _():
        sent(a_ref)

        @pl.when(col == 0)
        def _():
            sent(panel_in.at[0])

    @pl.when(core == 1)
    def _():
        @pl.when(pair == 0)
        def _():
            sent(panel_in)
            sent(panel_in.at[pl.ds(0, rows - 2)])

        for _ in range(2):
            sent(a_ref)
        sent(vecs)
        sent(images)
        sent(ends)

    sent(eig_cols.at[pl.ds(0, 7)])
    sent(eig_cols.at[pl.ds(0, rows // 2)])
    sent(psi_rows.at[pl.ds(0, 7)])

    def drain(step, carry):
        sent(parts_in.at[step, pl.ds(0, rows - 1)])
        return carry

    @pl.when(core == 1)
    def _():
        lax.fori_loop(0, PB, drain, 0)

    for n in range(2):
        sent(by_row.at[n, 0, pl.ds(0, rows - 1)])
        sent(by_col.at[n, 0, pl.ds(0, cols - 1)])
        sent(by_row.at[n, pl.ds(0, 7)])
        sent(by_col.at[n, pl.ds(0, 7)])
        sent(by_col.at[n, pl.ds(0, rows // 2)])


def reduce_and_rotate(psi, hpsi, eigvec, rows, cols):
    height, width = eigvec.shape
    tile = 128
    halves = height // tile
    tiles = rows * halves
    depth = cols * psi.shape[0]
    vmem = pl.BlockSpec(memory_space=pltpu.VMEM)
    block = pltpu.VMEM((height, width), jnp.float32)
    vectors = pltpu.VMEM((PB, tiles, tile), jnp.float32)
    laid = jax.ShapeDtypeStruct((height * width // tile, tile), jnp.float32)
    return pl.pallas_call(
        whole_kernel,
        out_shape=(
            laid,
            laid,
            jax.ShapeDtypeStruct((1, PB), jnp.float32),
            jax.ShapeDtypeStruct((1, PB), jnp.float32),
            jax.ShapeDtypeStruct((depth * width // tile, tile), psi.dtype),
        ),
        in_specs=[vmem] * 3,
        out_specs=(vmem,) * 5,
        scratch_shapes=[
            pltpu.VMEM((2, cols, rows, psi.shape[0], height), psi.dtype),
            pltpu.VMEM((2, rows, cols, psi.shape[0], width), psi.dtype),
            block,
            block,
            pltpu.VMEM((cols, *psi.shape), psi.dtype),
            pltpu.VMEM((rows, *eigvec.shape), eigvec.dtype),
            pltpu.VMEM((depth, width), jnp.float32),
            pltpu.VMEM((depth * width // tile, tile), jnp.float32),
            pltpu.VMEM((cols // 2, 2 * height, width), jnp.float32),
            pltpu.VMEM((rows, PB + 1, halves, tile), jnp.float32),
            pltpu.VMEM((PB + 1, tiles, tile), jnp.float32),
            vectors,
            vectors,
            pltpu.VMEM((tiles, tile), jnp.float32),
            pltpu.VMEM((2 * height, tile), jnp.float32),
            pltpu.VMEM((PB, 2 * halves, tile), jnp.float32),
            pltpu.VMEM((PB, rows, 2 * halves, tile), jnp.float32),
            pltpu.VMEM((tiles, tile), jnp.float32),
            pltpu.VMEM((2, 8, tile), jnp.float32),
            pltpu.SemaphoreType.DMA,
            pltpu.SemaphoreType.DMA((2, 2)),
            pltpu.SemaphoreType.DMA((2, 2, 9)),
            pltpu.SemaphoreType.DMA((2,)),
            pltpu.SemaphoreType.DMA((2, 6)),
            pltpu.SemaphoreType.DMA((3,)),
            pltpu.SemaphoreType.DMA((PB,)),
            pltpu.SemaphoreType.DMA((9,)),
            pltpu.SemaphoreType.DMA,
            pltpu.SemaphoreType.DMA((9,)),
            pltpu.SemaphoreType.DMA((4,)),
        ],
        compiler_params=pltpu.CompilerParams(
            collective_id=0, has_side_effects=True, vmem_limit_bytes=56 * 1024 * 1024
        ),
        name="whole",
    )(psi, hpsi, eigvec)


def on_device(psi, hpsi, eigvec):
    row_tiles, _, tile_size, col_tiles = eigvec.shape[:4]
    correlation, updated, diagonal, offdiag, rotated = reduce_and_rotate(
        psi,
        hpsi,
        eigvec.reshape(row_tiles * tile_size, col_tiles * tile_size),
        lax.axis_size("row"),
        lax.axis_size("col"),
    )
    tile_shape = (row_tiles, 1, tile_size, col_tiles, 1, tile_size)
    return (
        correlation.reshape(tile_shape),
        updated.reshape(tile_shape),
        diagonal.reshape(PB),
        offdiag.reshape(PB),
        rotated.reshape(-1, col_tiles, 1, tile_size),
    )


def solution(mesh):
    return jax.shard_map(
        on_device,
        mesh=mesh,
        in_specs=(
            P(("row", "col"), None),
            P(("row", "col"), None),
            P(None, "row", None, None, "col", None),
        ),
        out_specs=(
            P(None, "row", None, None, "col", None),
            P(None, "row", None, None, "col", None),
            P(),
            P(),
            P("row", None, "col", None),
        ),
        check_vma=False,
    )
```
